32 devices in a mesh: lat: 8 (over z, y), lon: 4 (over x, core).
Axes of the slice: x: 2, y: 2, z: 4, core: 2. Of those that a mesh axis runs over, the one named last changes fastest.
Arguments:
- grid_latent: bfloat16 [16384, 512], P(('lat', 'lon')), may hold values from -6 to 6
- grid_feat: bfloat16 [4, 65536], P(None, ('lat', 'lon')), may hold values from -6 to 6
- grid_sender: int32 [65536], P(('lat', 'lon')), may hold values from 0 to 511
- grid_owner: int32 [65536, 1], P(('lat', 'lon')), may hold values from 0 to 7; in each aligned block of 2048 rows (0 to 2047, 2048 to 4095, ...) at most 512 rows name the same one
- grid_node: int32 [65536], P(('lat', 'lon')), may hold values from 0 to 511
- mesh_latent: bfloat16 [4096, 512], P('lat', 'lon'), may hold values from -6 to 6
- mesh_edge: bfloat16 [32768, 512], P(('lat', 'lon')), may hold values from -6 to 6
- halo_send: int32 [64, 64], P('lat'), may hold values from 0 to 511
- mesh_sender: int32 [32768], P(('lat', 'lon')), may hold values from 0 to 1023
- mesh_receiver: int32 [32768], P(('lat', 'lon')), may hold values from 0 to 511
- enc_edge_in: bfloat16 [512, 512], P(None, 'lon'), may hold values from -0.25 to 0.25
- enc_feat_proj: bfloat16 [4, 512], replicated, may hold values from -3 to 3
- enc_edge_out: bfloat16 [512, 512], P(None, 'lon'), may hold values from -0.25 to 0.25
- enc_edge_bias: float32 [2, 512], replicated, may hold values from -1.5 to 1.5
- enc_edge_gain: float32 [512], replicated, may hold values from 0.25 to 1.75
- enc_node_in: bfloat16 [1024, 512], P(None, 'lon'), may hold values from -0.1875 to 0.1875
- enc_node_out: bfloat16 [512, 512], P('lon'), may hold values from -0.25 to 0.25
- enc_node_bias: float32 [2, 512], replicated, may hold values from -1.5 to 1.5
- enc_node_gain: float32 [512], replicated, may hold values from 0.25 to 1.75
- proc_edge_in: bfloat16 [1536, 512], P(None, 'lon'), may hold values from -0.15625 to 0.15625
- proc_edge_out: bfloat16 [512, 512], P(None, 'lon'), may hold values from -0.25 to 0.25
- proc_edge_bias: float32 [2, 512], replicated, may hold values from -1.5 to 1.5
- proc_edge_gain: float32 [512], replicated, may hold values from 0.25 to 1.75
- proc_node_in: bfloat16 [1024, 512], P(None, 'lon'), may hold values from -0.1875 to 0.1875
- proc_node_out: bfloat16 [512, 512], P('lon'), may hold values from -0.25 to 0.25
- proc_node_bias: float32 [2, 512], replicated, may hold values from -1.5 to 1.5
- proc_node_gain: float32 [512], replicated, may hold values from 0.25 to 1.75
Outputs:
- mesh_update: bfloat16 [4096, 512], P('lat', 'lon')
- edge_update: bfloat16 [32768, 512], P(('lat', 'lon'))
The draws below stay inside these ranges and needn't reach their ends.
Inputs may be any that keep to these rules, and one draw needn't show every extreme that they name: `grid_sender`: a row among the 512 grid rows of the device that holds the edge. `grid_owner`: among the 2048 edges of one device, at most 512 name the same partition, a bound that some block reaches. `halo_send`: nodes of the listing partition.
All inputs are finite; a program needn't handle non-finite values.
Results may differ from the reference program's by a relative error of at most 0.017.
Values may be sent and summed in bfloat16 or wider, within the bound.
No kernel may reach another device: no remote copies, remote signals or barrier semaphores. Data moves between devices by JAX's collectives and lax.ppermute only.
A program may use at most 128 MiB of HBM per device.

```python
import math
import jax
import jax.numpy as jnp
import numpy as np
from jax import lax

D = 512
EF = 4
DEG = 8
G_DEV = 512
MESH_DEV = 512
GE_DEV = 2048
CAP = 512
HCAP = 64
GRID = 16384
GRID_EDGES = 65536
MESH = 4096
MESH_EDGES = 32768
N_LAT = 8
N_LON = 4


def touch_ends(drawn, stream_key, least, high):
    extent = drawn.shape
    index_at = [jax.random.randint(jax.random.fold_in(stream_key, axis), (), 0, extent[axis]) for axis in range(len(extent))]
    drawn = drawn.at[tuple(index_at)].set(least)
    longest = extent.index(max(extent))
    index_at[longest] = (index_at[longest] + 1) % extent[longest]
    return drawn.at[tuple(index_at)].set(high)


def level_of(key, shape, shards, smallest, largest):
    level = 1.0
    for position, shards_of in shards:
        draws = jax.random.uniform(jax.random.fold_in(jax.random.fold_in(key, 6), position), (shards_of,), jnp.float32, smallest / len(shards), largest / len(shards))
        level = level * jnp.repeat(jnp.exp(draws), shape[position] // shards_of).reshape((-1,) + (1,) * (len(shape) - 1 - position))
    return level


def shared_out(rng, own, number, rows, number_of, top, limit, skew):
    sequence = jax.random.permutation(rng, number_of)
    crowded, usual = portions_of(number_of, rows * top, limit, skew, True), portions_of(number_of, rows * top, limit, skew, False)
    places = jnp.arange(number_of)

    def named(lengths, offset_by):
        used = int((lengths > 0).sum())
        fixed = max(1, used // 4)
        passed = fixed + (places - fixed + offset_by * (used - fixed)) % max(1, number_of - fixed)
        return jnp.zeros((number_of,), jnp.int32).at[sequence[jnp.where(places < fixed, places, passed)]].set(jnp.asarray(lengths, jnp.int32))

    lengths = jnp.where(number % 4 == 0, named(crowded, number // 4), named(usual, number - number // 4 - 1))
    mixed = jax.random.permutation(jax.random.fold_in(own, 3), number_of)
    donor, sink = mixed[0:number_of // 2 * 2:2], mixed[1:number_of // 2 * 2:2]
    margin = jnp.minimum(lengths[donor] - 1, limit - lengths[sink]) // 2
    margin = jnp.where((donor == sequence[0]) | (sink == sequence[0]) | (lengths[sink] == 0), 0, jnp.maximum(margin, 0))
    passed = jax.random.randint(jax.random.fold_in(own, 4), (number_of // 2,), 0, 1 << 20) % (margin + 1)
    lengths = lengths.at[donor].add(-passed).at[sink].add(passed)
    members = jnp.searchsorted(jnp.cumsum(lengths), jnp.arange(rows * top), side="right").astype(jnp.int32)
    grid = members.reshape(top, rows).T
    grid = grid[jax.random.permutation(jax.random.fold_in(own, 1), rows)]
    offset_by = jax.random.randint(jax.random.fold_in(own, 2), (rows, 1), 0, top)
    return jnp.take_along_axis(grid, (jnp.arange(top)[None, :] + offset_by) % top, axis=1)


def portions_of(count, total, bound, skew, full):
    loads = [(1 << 20) // math.isqrt(standing ** skew) + 1 for standing in range(1, count + 1)]
    largest = bound if full else min(bound, max(-(-total // count), total * loads[0] // sum(loads)))
    least = 1 if total - largest >= count - 1 else 0
    counts, spare = [largest] + [least] * (count - 1), total - largest - least * (count - 1)
    while spare > 0:
        free = [i for i in range(1, count) if counts[i] < largest] or [i for i in range(1, count) if counts[i] < bound]
        whole, budget = sum([loads[i] for i in free]), spare
        for i in free:
            extra = min(bound - counts[i], max(1, budget * loads[i] // whole), spare)
            counts[i] = counts[i] + extra
            spare = spare - extra
    return np.array(counts)


def scatter_about(own_key, shape, scale, bound, split=(), kind=jnp.bfloat16):
    entries = jax.random.normal(own_key, shape, jnp.float32) * scale
    if len(split) > 0:
        entries = level_of(own_key, shape, split, -0.22, 0.18) * entries
    return jnp.clip(entries, min=-bound, max=bound).astype(kind)


def setup_inputs(seed: int = 0) -> dict:
    streams_of = jax.random.split(jax.random.key(seed), 28)
    grid_latent = scatter_about(streams_of[0], (GRID, D), 1.0, 6.0, ((0, 32),))
    grid_feat = scatter_about(streams_of[1], (EF, GRID_EDGES), 1.0, 6.0, ((1, 32),))
    grid_sender = touch_ends(jax.random.randint(streams_of[2], (GRID_EDGES,), 0, G_DEV), jax.random.fold_in(streams_of[2], 1), 0, G_DEV - 1).astype(jnp.int32)
    grid_owner_keys = jax.random.split(jax.random.fold_in(streams_of[3], 1), GRID_EDGES // GE_DEV)
    grid_owner_turns = jax.random.permutation(jax.random.fold_in(streams_of[3], 3), GRID_EDGES // GE_DEV)
    grid_owner = jax.vmap(lambda own, number: shared_out(jax.random.fold_in(streams_of[3], 2), own, number, GE_DEV, N_LAT, 1, CAP, 2))(grid_owner_keys, grid_owner_turns).reshape((GRID_EDGES, 1))
    grid_node = touch_ends(jax.random.randint(streams_of[4], (GRID_EDGES,), 0, MESH_DEV), jax.random.fold_in(streams_of[4], 1), 0, MESH_DEV - 1).astype(jnp.int32)
    mesh_latent = scatter_about(streams_of[5], (MESH, D), 1.0, 6.0, ((0, 8), (1, 4)))
    mesh_edge = scatter_about(streams_of[6], (MESH_EDGES, D), 1.0, 6.0, ((0, 32),))
    halo_send = touch_ends(jax.random.randint(streams_of[7], (N_LAT * N_LAT, HCAP), 0, MESH_DEV), jax.random.fold_in(streams_of[7], 1), 0, MESH_DEV - 1).astype(jnp.int32)
    mesh_sender = touch_ends(jax.random.randint(streams_of[8], (MESH_EDGES,), 0, MESH_DEV + N_LAT * HCAP), jax.random.fold_in(streams_of[8], 1), 0, (MESH_DEV + N_LAT * HCAP) - 1).astype(jnp.int32)
    mesh_receiver = touch_ends(jax.random.randint(streams_of[9], (MESH_EDGES,), 0, MESH_DEV), jax.random.fold_in(streams_of[9], 1), 0, MESH_DEV - 1).astype(jnp.int32)
    enc_edge_in = scatter_about(streams_of[10], (D, D), D ** -0.5, 0.25, ((1, 4),))
    enc_feat_proj = scatter_about(streams_of[11], (EF, D), EF ** -0.5, 3.0)
    enc_edge_out = scatter_about(streams_of[12], (D, D), D ** -0.5, 0.25, ((1, 4),))
    enc_edge_bias = scatter_about(streams_of[13], (2, D), 0.3, 1.5, (), jnp.float32)
    enc_edge_gain = jnp.clip(1.0 + 0.15 * jax.random.normal(streams_of[14], (D,), jnp.float32), 0.25, 1.75)
    enc_node_in = scatter_about(streams_of[15], (2 * D, D), (2 * D) ** -0.5, 0.1875, ((1, 4),))
    enc_node_out = scatter_about(streams_of[16], (D, D), D ** -0.5, 0.25, ((0, 4),))
    enc_node_bias = scatter_about(streams_of[17], (2, D), 0.3, 1.5, (), jnp.float32)
    enc_node_gain = jnp.clip(1.0 + 0.15 * jax.random.normal(streams_of[18], (D,), jnp.float32), 0.25, 1.75)
    proc_edge_in = scatter_about(streams_of[19], (3 * D, D), (3 * D) ** -0.5, 0.15625, ((1, 4),))
    proc_edge_out = scatter_about(streams_of[20], (D, D), D ** -0.5, 0.25, ((1, 4),))
    proc_edge_bias = scatter_about(streams_of[21], (2, D), 0.3, 1.5, (), jnp.float32)
    proc_edge_gain = jnp.clip(1.0 + 0.15 * jax.random.normal(streams_of[22], (D,), jnp.float32), 0.25, 1.75)
    proc_node_in = scatter_about(streams_of[23], (2 * D, D), (2 * D) ** -0.5, 0.1875, ((1, 4),))
    proc_node_out = scatter_about(streams_of[24], (D, D), D ** -0.5, 0.25, ((0, 4),))
    proc_node_bias = scatter_about(streams_of[25], (2, D), 0.3, 1.5, (), jnp.float32)
    proc_node_gain = jnp.clip(1.0 + 0.15 * jax.random.normal(streams_of[26], (D,), jnp.float32), 0.25, 1.75)
    return {"grid_latent": grid_latent, "grid_feat": grid_feat, "grid_sender": grid_sender, "grid_owner": grid_owner, "grid_node": grid_node, "mesh_latent": mesh_latent, "mesh_edge": mesh_edge, "halo_send": halo_send, "mesh_sender": mesh_sender, "mesh_receiver": mesh_receiver, "enc_edge_in": enc_edge_in, "enc_feat_proj": enc_feat_proj, "enc_edge_out": enc_edge_out, "enc_edge_bias": enc_edge_bias, "enc_edge_gain": enc_edge_gain, "enc_node_in": enc_node_in, "enc_node_out": enc_node_out, "enc_node_bias": enc_node_bias, "enc_node_gain": enc_node_gain, "proc_edge_in": proc_edge_in, "proc_edge_out": proc_edge_out, "proc_edge_bias": proc_edge_bias, "proc_edge_gain": proc_edge_gain, "proc_node_in": proc_node_in, "proc_node_out": proc_node_out, "proc_node_bias": proc_node_bias, "proc_node_gain": proc_node_gain}


def layer_norm(values, norm_gain, offsets):
    average = lax.optimization_barrier(jnp.mean(values, axis=-1, keepdims=True))
    centred = values - average
    spread = lax.optimization_barrier(jnp.mean(centred * centred, axis=-1, keepdims=True))
    return centred * lax.rsqrt(spread + 1e-05) * norm_gain + offsets

def node_network(base, aggregate, weight_in, weight_out, biases, norm_gain):
    inputs = jnp.concatenate([base, aggregate], 1)
    hidden = jax.nn.silu(jnp.dot(inputs, weight_in, preferred_element_type=jnp.float32) + biases[0]).astype(jnp.bfloat16)
    raw_out = jnp.dot(hidden, weight_out, preferred_element_type=jnp.float32)
    return (base.astype(jnp.float32) + layer_norm(raw_out, norm_gain, biases[1])).astype(jnp.bfloat16)

def reference(grid_latent, grid_feat, grid_sender, grid_owner, grid_node, mesh_latent, mesh_edge, halo_send, mesh_sender, mesh_receiver, enc_edge_in, enc_feat_proj, enc_edge_out, enc_edge_bias, enc_edge_gain, enc_node_in, enc_node_out, enc_node_bias, enc_node_gain, proc_edge_in, proc_edge_out, proc_edge_bias, proc_edge_gain, proc_node_in, proc_node_out, proc_node_bias, proc_node_gain):
    device_count = N_LAT * N_LON
    mesh_count = MESH_DEV * N_LAT
    owner_column = grid_owner[:, 0]

    def encode(summed, device):
        first = device * GE_DEV
        senders = lax.dynamic_slice_in_dim(grid_sender, first, GE_DEV) + device * G_DEV
        source_rows = jnp.take(grid_latent, senders, axis=0)
        feats = lax.dynamic_slice_in_dim(grid_feat, first, GE_DEV, 1)
        feat_term = jnp.dot(feats.T, enc_feat_proj, preferred_element_type=jnp.float32) + enc_edge_bias[0]
        pre_act = jnp.dot(source_rows, enc_edge_in, preferred_element_type=jnp.float32) + feat_term
        hidden = jax.nn.silu(pre_act).astype(jnp.bfloat16)
        raw_out = jnp.dot(hidden, enc_edge_out.T, preferred_element_type=jnp.float32)
        messages = layer_norm(raw_out, enc_edge_gain, enc_edge_bias[1])
        owners = lax.dynamic_slice_in_dim(owner_column, first, GE_DEV)
        nodes = lax.dynamic_slice_in_dim(grid_node, first, GE_DEV)
        return (summed.at[owners * MESH_DEV + nodes].add(messages), device)
    start_sum = jnp.zeros((mesh_count, D), jnp.float32)
    gathered, leftover = lax.scan(encode, start_sum, jnp.arange(device_count, dtype=jnp.int32))
    mesh_mid = node_network(mesh_latent, gathered.astype(jnp.bfloat16), enc_node_in, enc_node_out, enc_node_bias, enc_node_gain)
    halo_table = halo_send.reshape(N_LAT, N_LAT, HCAP)
    part_edges = MESH_DEV * DEG

    def process(part):
        local = lax.dynamic_slice_in_dim(mesh_mid, part * MESH_DEV, MESH_DEV)
        picks = lax.dynamic_index_in_dim(halo_table, part, 1, keepdims=False)
        global_rows = (jnp.arange(N_LAT, dtype=jnp.int32)[:, None] * MESH_DEV + picks).reshape(-1)
        table = jnp.concatenate([local, jnp.take(mesh_mid, global_rows, axis=0)], 0)
        first = part * part_edges
        edges = lax.dynamic_slice_in_dim(mesh_edge, first, part_edges)
        senders = lax.dynamic_slice_in_dim(mesh_sender, first, part_edges)
        receivers = lax.dynamic_slice_in_dim(mesh_receiver, first, part_edges)
        sender_rows = jnp.take(table, senders, axis=0)
        receiver_rows = jnp.take(local, receivers, axis=0)
        pre_act = jnp.dot(edges, proc_edge_in[:D], preferred_element_type=jnp.float32)
        pre_act = pre_act + jnp.dot(sender_rows, proc_edge_in[D:2 * D], preferred_element_type=jnp.float32)
        pre_act = pre_act + jnp.dot(receiver_rows, proc_edge_in[2 * D:], preferred_element_type=jnp.float32)
        hidden = jax.nn.silu(pre_act + proc_edge_bias[0]).astype(jnp.bfloat16)
        raw_out = jnp.dot(hidden, proc_edge_out.T, preferred_element_type=jnp.float32)
        updated = (edges.astype(jnp.float32) + layer_norm(raw_out, proc_edge_gain, proc_edge_bias[1])).astype(jnp.bfloat16)
        onehot = (jnp.arange(MESH_DEV, dtype=jnp.int32)[:, None] == receivers[None, :]).astype(jnp.bfloat16)
        incoming = jnp.dot(onehot, updated, preferred_element_type=jnp.float32)
        return (updated, incoming)
    edge_blocks, incoming_blocks = lax.map(process, jnp.arange(N_LAT, dtype=jnp.int32))
    edge_update = edge_blocks.reshape(-1, D)
    incoming = incoming_blocks.reshape(-1, D)
    mesh_update = node_network(mesh_mid, incoming.astype(jnp.bfloat16), proc_node_in, proc_node_out, proc_node_bias, proc_node_gain)
    return (mesh_update, edge_update)
```

```python
import functools
import jax
import jax.numpy as jnp
from jax import lax
from jax.experimental import pallas as pl
from jax.experimental.pallas import tpu as pltpu
from jax.sharding import PartitionSpec as P

F32 = jnp.float32
BF16 = jnp.bfloat16
I32 = jnp.int32
SPLIT = 32
CHUNK = 256
META = 16

VMEM = pl.BlockSpec(memory_space=pltpu.VMEM)
SMEM = pl.BlockSpec(memory_space=pltpu.SMEM)


def dot(a, b, ca=1, cb=0):
    return lax.dot_general(a, b, (((ca,), (cb,)), ((), ())), preferred_element_type=F32)


def cost(flops, nbytes):
    return pl.CostEstimate(flops=int(flops), bytes_accessed=int(nbytes), transcendentals=0)


def call(kernel, out_shape, n_in, flops, scratch=(), smem=0, n_out=1):
    return pl.pallas_call(
        kernel,
        out_shape=out_shape,
        in_specs=[SMEM] * smem + [VMEM] * (n_in - smem),
        out_specs=VMEM if n_out == 1 else [VMEM] * n_out,
        scratch_shapes=list(scratch),
        cost_estimate=cost(flops, 4 << 20),
        compiler_params=pltpu.CompilerParams(vmem_limit_bytes=56 << 20),
    )


def silu(t):
    return t / (1.0 + jnp.exp(-t))


def normed(raw, gain, offset, axis):
    width = raw.shape[axis]
    average = jnp.sum(raw, axis=axis, keepdims=True) * (1.0 / width)
    centred = raw - average
    spread = jnp.sum(centred * centred, axis=axis, keepdims=True) * (1.0 / width)
    return centred * lax.rsqrt(spread + 1e-05) * gain + offset


def sort_kernel(lat_count, mesh_rows, owner_ref, sender_ref, node_ref, feat_ref, key_ref, send_ref, feats_ref, start_ref):
    edges = owner_ref.shape[1]
    owner = owner_ref[...]
    parts = lax.broadcasted_iota(I32, (lat_count, edges), 0)
    hits = jnp.where(parts == owner, 1.0, 0.0)
    lane = lax.broadcasted_iota(I32, (lat_count, edges), 1)
    count = hits
    step = 1
    while step < edges:
        count = count + jnp.where(lane >= step, pltpu.roll(count, step, 1), 0.0)
        step *= 2
    first = jnp.sum(jnp.where(owner < parts, 1.0, 0.0), axis=1, keepdims=True)
    place = jnp.sum(hits * (first + count - hits), axis=0, keepdims=True).astype(I32)
    start_ref[...] = jnp.broadcast_to(first, start_ref.shape).astype(I32)
    sender = sender_ref[...]
    node = node_ref[...]
    digits = [sender // SPLIT, sender % SPLIT, node // SPLIT, node % SPLIT, owner]
    rows = [d.astype(F32) for d in digits] + [feat_ref[...].astype(F32)]
    used = len(digits) + feat_ref.shape[0]
    meta = jnp.concatenate(rows + [jnp.ones((META - used, edges), F32)], 0).astype(BF16)
    block = 512

    @pl.loop(0, edges // block)
    def _(i):
        spot = lax.broadcasted_iota(I32, (block, edges), 0) + i * block
        perm = jnp.where(spot == place, 1.0, 0.0).astype(BF16)
        moved = dot(meta, perm, 1, 1)
        at = pl.ds(pl.multiple_of(i * block, block), block)
        ints = moved.astype(I32)
        send_ref[:, at] = ints[0:1] * SPLIT + ints[1:2]
        key_ref[:, at] = ints[4:5] * mesh_rows + ints[2:3] * SPLIT + ints[3:4]
        feats_ref[:, at] = moved.astype(BF16)


def message_kernel(n_feat, lon_ref, rows_ref, send_ref, feats_ref, proj_ref, bias_ref, gain_ref, w0, w1, w2, w3, out_ref, win, wout, proj):
    width = rows_ref.shape[1]
    quarter = w0.shape[1]
    lon = lon_ref[0]
    for j, w in enumerate((w0, w1, w2, w3)):
        win[:, j * quarter : (j + 1) * quarter] = w[0:width, :]
        wout[:, j * quarter : (j + 1) * quarter] = w[width : 2 * width, :]
        at = pl.ds(pl.multiple_of((lon ^ j) * quarter, quarter), quarter)
        bias = bias_ref[0:1, at]
        high = bias.astype(BF16).astype(F32)
        mid = (bias - high).astype(BF16).astype(F32)
        low = bias - high - mid
        used = META - 5 - n_feat
        proj[:, j * quarter : (j + 1) * quarter] = jnp.concatenate(
            [jnp.zeros((5, quarter), F32), proj_ref[:, at].astype(F32), high, mid, low, jnp.zeros((used - 3, quarter), F32)], 0
        ).astype(BF16)
    rows = rows_ref[...]
    table = dot(win[...], rows, 0, 1).astype(BF16)
    columns = jnp.transpose(gain_ref[...])
    gain, offset = columns[:, 0:1], columns[:, 1:2]
    edges = send_ref.shape[1]
    block = CHUNK

    @pl.loop(0, edges // block)
    def _(i):
        at = pl.ds(pl.multiple_of(i * block, block), block)
        source = lax.broadcasted_iota(I32, (rows.shape[0], block), 0)
        pick = jnp.where(source == send_ref[:, at], 1.0, 0.0).astype(BF16)
        pre = dot(table, pick) + dot(proj[...], feats_ref[:, at], 0, 0)
        hidden = silu(pre).astype(BF16)
        raw = dot(wout[...], hidden)
        out_ref[i] = normed(raw, gain, offset, 0).astype(BF16)


def sums_kernel(mesh_rows, edges, start_ref, core_ref, key_ref, msg_ref, out_ref):
    part = pl.program_id(0)
    parts = pl.num_programs(0)
    begin = start_ref[part]
    end = jnp.where(part + 1 < parts, start_ref[jnp.minimum(part + 1, parts - 1)], edges)
    quarter = out_ref.shape[2]
    core = core_ref[0]
    half = 2 * quarter
    row = lax.broadcasted_iota(I32, (half, CHUNK), 0)
    node = row + jnp.where(row >= quarter, quarter, 0) + core * quarter + part * mesh_rows

    def body(i, total):
        pick = jnp.where(node == key_ref[i], 1.0, 0.0).astype(BF16)
        return total + dot(pick, msg_ref[i], 1, 1)

    total = lax.fori_loop(
        begin // CHUNK, (end + CHUNK - 1) // CHUNK, body, jnp.zeros((half, msg_ref.shape[1]), F32)
    ).astype(BF16)
    out_ref[0, 0] = total[:quarter]
    out_ref[0, 1] = total[quarter:]


def node_sums(starts, core, keys, messages, lat_count, mesh_rows, edges):
    quarter = mesh_rows // 4
    chunks, width, _ = messages.shape
    return pl.pallas_call(
        functools.partial(sums_kernel, mesh_rows, edges),
        out_shape=jax.ShapeDtypeStruct((lat_count, 2, quarter, width), BF16),
        grid=(lat_count,),
        in_specs=[SMEM, SMEM, pl.BlockSpec((chunks, 1, CHUNK), lambda p: (0, 0, 0)), pl.BlockSpec((chunks, width, CHUNK), lambda p: (0, 0, 0))],
        out_specs=pl.BlockSpec((1, 2, quarter, width), lambda p: (p, 0, 0, 0)),
        cost_estimate=cost(edges * mesh_rows * width * 2, 8 << 20),
        compiler_params=pltpu.CompilerParams(vmem_limit_bytes=48 << 20),
    )(starts, core, keys, messages)


def node_kernel(full_base, lon_ref, *refs):
    n_base = 1 if full_base else 4
    bases = refs[:n_base]
    agg_ref, bias_ref, gain_ref, w0, w1, w2, w3, out_ref, base, win, wout = refs[n_base:]
    width = agg_ref.shape[-1]
    quarter = w0.shape[1]
    lon = lon_ref[0]
    biases = []
    for j, w in enumerate((w0, w1, w2, w3)):
        win[:, j * quarter : (j + 1) * quarter] = w[0 : 2 * width, :]
        for m in range(width // quarter):
            wout[j * quarter : (j + 1) * quarter, m * quarter : (m + 1) * quarter] = w[
                2 * width + m * quarter : 2 * width + (m + 1) * quarter, :
            ]
        at = pl.ds(pl.multiple_of((lon ^ j) * quarter, quarter), quarter)
        biases.append(bias_ref[0:1, at])
        if not full_base:
            base[:, at] = bases[j][...]
    if full_base:
        base[...] = bases[0][...]
    total = agg_ref[0].astype(F32)
    for k in range(1, agg_ref.shape[0]):
        total = total + agg_ref[k].astype(F32)
    own = base[...]
    pre = dot(own, win[0:width, :]) + dot(total.astype(BF16), win[width:, :]) + jnp.concatenate(biases, 1)
    raw = dot(silu(pre).astype(BF16), wout[...])
    out_ref[...] = (own.astype(F32) + normed(raw, gain_ref[...], bias_ref[1:2, :], 1)).astype(BF16)


def node_network(lon, bases, aggregate, biases, gain, pieces):
    rows, width = aggregate.shape[1:]
    kernel = functools.partial(node_kernel, len(bases) == 1)
    scratch = [pltpu.VMEM((rows, width), BF16), pltpu.VMEM((2 * width, width), BF16), pltpu.VMEM((width, width), BF16)]
    return call(
        kernel, jax.ShapeDtypeStruct((rows, width), BF16), 8 + len(bases), 6 * rows * width * width, scratch, 1
    )(lon, *bases, aggregate, biases, gain[None, :], *pieces)


def pick_kernel(index_ref, table_ref, out_ref):
    lane = lax.broadcasted_iota(I32, (index_ref.shape[0], table_ref.shape[0]), 1)
    pick = jnp.where(lane == index_ref[...], 1.0, 0.0).astype(BF16)
    out_ref[...] = dot(pick, table_ref[...]).astype(BF16)


def near_kernel(lon_ref, edge_ref, mid_ref, sender_ref, receiver_ref, bias_ref, w0, w1, w2, w3, out_ref, win):
    width = mid_ref.shape[1]
    quarter = w0.shape[1]
    lon = lon_ref[0]
    biases = []
    for j, w in enumerate((w0, w1, w2, w3)):
        win[:, j * quarter : (j + 1) * quarter] = w[0 : 3 * width, :]
        at = pl.ds(pl.multiple_of((lon ^ j) * quarter, quarter), quarter)
        biases.append(bias_ref[0:1, at])
    bias = jnp.concatenate(biases, 1)
    rows = mid_ref.shape[0]
    sent = dot(mid_ref[...], win[width : 2 * width, :]).astype(BF16)
    got = dot(mid_ref[...], win[2 * width :, :]).astype(BF16)
    edges = edge_ref.shape[0]
    block = 256

    @pl.loop(0, edges // block)
    def _(i):
        at = pl.ds(pl.multiple_of(i * block, block), block)
        lane = lax.broadcasted_iota(I32, (block, rows), 1)
        pick_s = jnp.where(lane == sender_ref[at, :], 1.0, 0.0).astype(BF16)
        pick_r = jnp.where(lane == receiver_ref[at, :], 1.0, 0.0).astype(BF16)
        out_ref[at, :] = dot(edge_ref[at, :], win[0:width, :]) + dot(pick_s, sent) + dot(pick_r, got) + bias


def far_kernel(pre_ref, edge_ref, halo_ref, sender_ref, receiver_ref, bias_ref, gain_ref, w0, w1, w2, w3, new_ref, sum_ref, total, win, wout):
    width = halo_ref.shape[1]
    quarter = w0.shape[1]
    for j, w in enumerate((w0, w1, w2, w3)):
        win[:, j * quarter : (j + 1) * quarter] = w[width : 2 * width, :]
        wout[:, j * quarter : (j + 1) * quarter] = w[3 * width : 4 * width, :]
    rows = halo_ref.shape[0]
    mesh_rows = sum_ref.shape[0]
    sent = dot(halo_ref[...], win[...]).astype(BF16)
    edges = edge_ref.shape[0]
    block = 256
    total[...] = jnp.zeros_like(total)

    @pl.loop(0, edges // block)
    def _(i):
        at = pl.ds(pl.multiple_of(i * block, block), block)
        lane = lax.broadcasted_iota(I32, (block, rows), 1) + mesh_rows
        pick = jnp.where(lane == sender_ref[at, :], 1.0, 0.0).astype(BF16)
        hidden = silu(pre_ref[at, :] + dot(pick, sent)).astype(BF16)
        raw = dot(hidden, wout[...], 1, 1)
        new = (edge_ref[at, :].astype(F32) + normed(raw, gain_ref[...], bias_ref[1:2, :], 1)).astype(BF16)
        new_ref[at, :] = new
        node = lax.broadcasted_iota(I32, (mesh_rows, block), 0)
        onto = jnp.where(node == receiver_ref[:, at], 1.0, 0.0).astype(BF16)
        total[...] += dot(onto, new)

    sum_ref[...] = total[...].astype(BF16)


def take(values, index, axis):
    return lax.dynamic_index_in_dim(values, index, axis, keepdims=False)


def plus(*values):
    total = values[0].astype(F32)
    for v in values[1:]:
        total = total + v.astype(F32)
    return total.astype(BF16)


def local(
    grid_latent,
    grid_feat,
    grid_sender,
    grid_owner,
    grid_node,
    mesh_latent,
    mesh_edge,
    halo_send,
    mesh_sender,
    mesh_receiver,
    enc_edge_in,
    enc_feat_proj,
    enc_edge_out,
    enc_edge_bias,
    enc_edge_gain,
    enc_node_in,
    enc_node_out,
    enc_node_bias,
    enc_node_gain,
    proc_edge_in,
    proc_edge_out,
    proc_edge_bias,
    proc_edge_gain,
    proc_node_in,
    proc_node_out,
    proc_node_bias,
    proc_node_gain,
):
    lat_count = lax.axis_size("lat")
    lat = lax.axis_index("lat")
    lon = lax.axis_index("lon")
    core, side = lon % 2, lon // 2
    low = lat % 2
    lon1 = lon.astype(I32)[None]
    width = grid_latent.shape[1]
    quarter = mesh_latent.shape[1]
    mesh_rows = mesh_latent.shape[0]
    node_rows = mesh_rows // 4
    edges = grid_sender.shape[0]

    def hop(values, axis, flip):
        size = lax.axis_size(axis)
        return lax.ppermute(values, axis, [(i, i ^ flip) for i in range(size)])

    def spread(shard):
        across = hop(shard, "lon", 2)
        return (shard, hop(shard, "lon", 1), across, hop(across, "lon", 1))

    def lie(weight):
        return jnp.concatenate([weight[:, m * quarter : (m + 1) * quarter] for m in range(weight.shape[1] // quarter)], 0)

    enc_pieces = spread(jnp.concatenate([enc_edge_in, enc_edge_out], 0))
    node_pieces = spread(jnp.concatenate([enc_node_in, lie(enc_node_out)], 0))
    edge_pieces = spread(jnp.concatenate([proc_edge_in, proc_edge_out], 0))
    last_pieces = spread(jnp.concatenate([proc_node_in, lie(proc_node_out)], 0))

    def own_rows(flip):
        rows = lax.dynamic_slice_in_dim(mesh_latent, (lon ^ flip) * node_rows, node_rows, 0)
        return rows if flip == 0 else hop(rows, "lon", flip)

    base_pieces = tuple(own_rows(flip) for flip in range(4))

    keys, senders, feats, starts = call(
        functools.partial(sort_kernel, lat_count, mesh_rows),
        [
            jax.ShapeDtypeStruct((1, edges), I32),
            jax.ShapeDtypeStruct((1, edges), I32),
            jax.ShapeDtypeStruct((META, edges), BF16),
            jax.ShapeDtypeStruct((lat_count, 128), I32),
        ],
        4,
        2 * META * edges * edges * 8,
        n_out=4,
    )(grid_owner.reshape(1, edges), grid_sender[None, :], grid_node[None, :], grid_feat)
    starts = starts[:, 0]
    keys = keys.reshape(edges // CHUNK, 1, CHUNK)
    enc_norm = jnp.concatenate(
        [enc_edge_gain[None, :], enc_edge_bias[1:2], jnp.zeros((6, width), F32)], 0
    )
    messages = call(
        functools.partial(message_kernel, grid_feat.shape[0]),
        jax.ShapeDtypeStruct((edges // CHUNK, width, CHUNK), BF16),
        11,
        4 * edges * width * width,
        [pltpu.VMEM((width, width), BF16), pltpu.VMEM((width, width), BF16), pltpu.VMEM((META, width), BF16)],
        1,
    )(lon1, grid_latent, senders, feats, enc_feat_proj, enc_edge_bias, enc_norm, *enc_pieces)

    away = node_sums(starts, (1 - core).astype(I32)[None], keys, messages, lat_count, mesh_rows, edges)
    came = hop(away, "lon", 1)
    kept = node_sums(starts, core.astype(I32)[None], keys, messages, lat_count, mesh_rows, edges)
    tall = lat_count // 2
    shape = (tall, 2, 2, node_rows, width)
    came, kept = came.reshape(shape), kept.reshape(shape)
    half = node_rows // 2

    def cut(rows, low_at=None, side_at=None):
        def of(v):
            v = v[:, :, :, rows]
            return take(v, side_at, 2) if low_at is None else take(v, low_at, 1)

        return plus(of(kept), of(came))

    first, second = slice(0, half), slice(half, node_rows)
    got_x = hop(cut(first, side_at=1 - side), "lon", 2)
    got_y = hop(cut(second, low_at=1 - low), "lat", 1)
    sum_x = plus(cut(first, side_at=side), got_x)
    got_xy = hop(take(sum_x, 1 - low, 1), "lat", 1)
    sum_y = plus(cut(second, low_at=low), got_y)
    got_yx = hop(take(sum_y, 1 - side, 1), "lon", 2)
    summed = jnp.concatenate([plus(take(sum_x, low, 1), got_xy), plus(take(sum_y, side, 1), got_yx)], 1)
    groups = [[2 * i + b for i in range(tall)] for b in range(2)]
    partial = lax.all_to_all(summed, "lat", 0, 0, axis_index_groups=groups, tiled=True)

    mid = node_network(lon1, base_pieces, partial, enc_node_bias, enc_node_gain, node_pieces)
    mid_all = lax.all_gather(mid, "lon", axis=0, tiled=True)

    listed = halo_send.size
    halo_cap = halo_send.shape[1]
    outgoing = call(
        pick_kernel, jax.ShapeDtypeStruct((listed, width), BF16), 2, 2 * listed * mesh_rows * width
    )(halo_send.reshape(listed, 1), mid_all)
    received = lax.all_to_all(outgoing.reshape(lat_count, halo_cap, width), "lat", 0, 0, tiled=True).reshape(listed, width)

    local_edges = mesh_edge.shape[0]
    sender_col = mesh_sender.reshape(local_edges, 1)
    receiver_col = mesh_receiver.reshape(local_edges, 1)
    near = call(
        near_kernel,
        jax.ShapeDtypeStruct((local_edges, width), F32),
        10,
        2 * local_edges * width * (width + 2 * mesh_rows),
        [pltpu.VMEM((3 * width, width), BF16)],
        1,
    )(lon1, mesh_edge, mid_all, sender_col, receiver_col, proc_edge_bias, *edge_pieces)
    edge_update, incoming = call(
        far_kernel,
        [jax.ShapeDtypeStruct((local_edges, width), BF16), jax.ShapeDtypeStruct((mesh_rows, width), BF16)],
        11,
        2 * local_edges * width * (width + listed + mesh_rows),
        [pltpu.VMEM((mesh_rows, width), F32), pltpu.VMEM((width, width), BF16), pltpu.VMEM((width, width), BF16)],
        n_out=2,
    )(near, mesh_edge, received, sender_col, mesh_receiver[None, :], proc_edge_bias, proc_edge_gain[None, :], *edge_pieces)

    incoming = incoming.reshape(2, 2, node_rows, width)
    came = hop(take(incoming, 1 - core, 1), "lon", 1)
    mine = take(incoming, core, 1)
    got = hop(plus(take(mine, 1 - side, 0), take(came, 1 - side, 0)), "lon", 2)
    parts = jnp.stack([take(mine, side, 0), take(came, side, 0), got], 0)
    new = node_network(lon1, (mid,), parts, proc_node_bias, proc_node_gain, last_pieces)
    spread_out = jnp.stack([new[:, m * quarter : (m + 1) * quarter] for m in range(4)], 0)
    mesh_update = lax.all_to_all(spread_out, "lon", 0, 0, tiled=True).reshape(mesh_rows, quarter)
    return (mesh_update, edge_update)


def solution(mesh):
    both = ("lat", "lon")
    placed = (
        P(both, None),
        P(None, both),
        P(both),
        P(both, None),
        P(both),
        P("lat", "lon"),
        P(both, None),
        P("lat", None),
        P(both),
        P(both),
        P(None, "lon"),
        P(),
        P(None, "lon"),
        P(),
        P(),
        P(None, "lon"),
        P("lon", None),
        P(),
        P(),
        P(None, "lon"),
        P(None, "lon"),
        P(),
        P(),
        P(None, "lon"),
        P("lon", None),
        P(),
        P(),
    )
    return jax.shard_map(
        local,
        mesh=mesh,
        in_specs=placed,
        out_specs=(P("lat", "lon"), P(both, None)),
        check_vma=False,
    )
```

```python
import functools
import jax
import jax.numpy as jnp
from jax import lax
from jax.experimental import pallas as pl
from jax.experimental.pallas import tpu as pltpu
from jax.sharding import PartitionSpec as P


F32 = jnp.float32
BF16 = jnp.bfloat16
I32 = jnp.int32
SPLIT = 32
CHUNK = 256
LANES = 128
WINDOW = 4
GRANT = 16 << 20
FULL = 59 << 20
META = 16

VMEM = pl.BlockSpec(memory_space=pltpu.VMEM)
SMEM = pl.BlockSpec(memory_space=pltpu.SMEM)
HBM = pl.BlockSpec(memory_space=pltpu.HBM)


def dot(a, b, ca=1, cb=0):
    return lax.dot_general(a, b, (((ca,), (cb,)), ((), ())), preferred_element_type=F32)


def cost(flops, nbytes):
    return pl.CostEstimate(flops=int(flops), bytes_accessed=int(nbytes), transcendentals=0)


def call(kernel, out_shape, specs, flops, scratch=(), grant=GRANT):
    many = isinstance(out_shape, list)
    return pl.pallas_call(
        kernel,
        out_shape=out_shape,
        in_specs=specs,
        out_specs=[VMEM] * len(out_shape) if many else VMEM,
        scratch_shapes=list(scratch),
        cost_estimate=cost(flops, 4 << 20),
        compiler_params=pltpu.CompilerParams(vmem_limit_bytes=grant),
    )


def silu(t):
    return 0.5 * t * (1.0 + jnp.tanh(0.5 * t))


def normed(raw, gain, offset, axis):
    width = raw.shape[axis]
    average = jnp.sum(raw, axis=axis, keepdims=True) * (1.0 / width)
    centred = raw - average
    spread = jnp.sum(centred * centred, axis=axis, keepdims=True) * (1.0 / width)
    return centred * lax.rsqrt(spread + 1e-05) * gain + offset


def columns_of(rows):
    height, width = rows.shape
    rows = rows.astype(F32)
    if height % 8:
        rows = jnp.concatenate([rows, jnp.zeros((8 - height % 8, width), F32)], 0)
    if width % LANES:
        rows = jnp.concatenate([rows, jnp.zeros((rows.shape[0], LANES - width % LANES), F32)], 1)
    return jnp.transpose(rows)


def open_kernel(
    lat_count,
    mesh_rows,
    owner_hbm,
    sender_hbm,
    node_hbm,
    feat_hbm,
    halo_hbm,
    from_hbm,
    to_hbm,
    latent,
    node_in,
    node_out,
    edge_in,
    edge_out,
    last_in,
    last_out,
    table_ref,
    meta_ref,
    ends_ref,
    asked_ref,
    base0,
    base1,
    base2,
    base3,
    node_pack,
    edge_pack,
    last_pack,
    owner_ref,
    sender_ref,
    node_ref,
    feat_ref,
    halo_ref,
    from_ref,
    to_ref,
    first_sem,
    sem,
):
    lon = lax.axis_index("lon")
    quarter = base0.shape[1]
    rows = base0.shape[0]
    inputs = (owner_hbm, sender_hbm, node_hbm, feat_hbm, halo_hbm, from_hbm, to_hbm)
    held = (owner_ref, sender_ref, node_ref, feat_ref, halo_ref, from_ref, to_ref)
    early = [pltpu.make_async_copy(a, b, first_sem.at[k]) for k, (a, b) in enumerate(zip(inputs, held))]
    late = []

    def bring(source, target):
        late.append(pltpu.make_async_copy(source, target, sem.at[len(late)]))

    for j, base in enumerate((base0, base1, base2, base3)):
        bring(latent.at[pl.ds(pl.multiple_of((lon ^ j) * rows, rows), rows), :], base)
    for w_in, w_out, pack in ((node_in, node_out, node_pack), (last_in, last_out, last_pack)):
        depth = w_in.shape[0]
        bring(w_in, pack.at[pl.ds(0, depth), :])
        for m in range(w_out.shape[1] // quarter):
            bring(w_out.at[:, pl.ds(m * quarter, quarter)], pack.at[pl.ds(depth + m * quarter, quarter), :])
    bring(edge_in, edge_pack.at[pl.ds(0, edge_in.shape[0]), :])
    bring(edge_out, edge_pack.at[pl.ds(edge_in.shape[0], edge_out.shape[0]), :])
    for copy in early + late:
        copy.start()
    for copy in early:
        copy.wait()
    ends_ref[...] = columns_of(jnp.concatenate([from_ref[...].astype(F32), to_ref[...].astype(F32)], 0)).astype(I32)
    asked = columns_of(halo_ref[...]).astype(I32)
    cap = halo_ref.shape[1]
    for p in range(lat_count):
        asked_ref[p * cap : (p + 1) * cap, :] = asked[0:cap, p : p + 1]
    edges = owner_ref.shape[1]
    owner = owner_ref[...]
    parts = lax.broadcasted_iota(I32, (lat_count, edges), 0)
    hits = jnp.where(parts == owner, 1.0, 0.0)
    lane = lax.broadcasted_iota(I32, (lat_count, edges), 1)
    count = hits
    step = 1
    while step < edges:
        count = count + jnp.where(lane >= step, pltpu.roll(count, step, 1), 0.0)
        step *= 2
    first = jnp.sum(jnp.where(owner < parts, 1.0, 0.0), axis=1, keepdims=True)
    place = jnp.sum(hits * (first + count - hits), axis=0, keepdims=True).astype(I32)
    key_rows = edges // LANES
    table_ref[key_rows:, :] = jnp.broadcast_to(first, (lat_count, LANES)).astype(I32)
    sender = sender_ref[...]
    node = node_ref[...]
    digits = [sender // SPLIT, sender % SPLIT, node // SPLIT, node % SPLIT, owner]
    rows = [d.astype(F32) for d in digits] + [feat_ref[...].astype(F32)]
    used = len(digits) + feat_ref.shape[0]
    meta = jnp.concatenate(rows + [jnp.ones((META - used, edges), F32)], 0).astype(BF16)
    for i in range(edges // CHUNK):
        spot = lax.broadcasted_iota(I32, (CHUNK, edges), 0) + i * CHUNK
        perm = jnp.where(spot == place, 1.0, 0.0).astype(BF16)
        moved = dot(meta, perm, 1, 1)
        meta_ref[i * CHUNK : (i + 1) * CHUNK, :] = jnp.transpose(moved).astype(BF16)
        key = moved[4:5] * float(mesh_rows) + moved[2:3] * float(SPLIT) + moved[3:4]
        for k in range(CHUNK // LANES):
            row = i * (CHUNK // LANES) + k
            table_ref[row : row + 1, :] = key[:, k * LANES : (k + 1) * LANES].astype(I32)
    for copy in late:
        copy.wait()


def message_kernel(n_feat, rows_ref, meta_ref, proj_ref, bias_ref, gain_ref, w0, w1, w2, w3, v0, v1, v2, v3, out_ref, win, wout, proj):
    quarter = w0.shape[1]
    lon = lax.axis_index("lon")
    for j, (w, v) in enumerate(((w0, v0), (w1, v1), (w2, v2), (w3, v3))):
        win[:, j * quarter : (j + 1) * quarter] = w[...]
        wout[:, j * quarter : (j + 1) * quarter] = v[...]
        at = pl.ds(pl.multiple_of((lon ^ j) * quarter, quarter), quarter)
        bias = bias_ref[0:1, at]
        high = bias.astype(BF16).astype(F32)
        mid = (bias - high).astype(BF16).astype(F32)
        low = bias - high - mid
        used = META - 5 - n_feat
        proj[:, j * quarter : (j + 1) * quarter] = jnp.concatenate(
            [jnp.zeros((5, quarter), F32), proj_ref[:, at].astype(F32), high, mid, low, jnp.zeros((used - 3, quarter), F32)], 0
        ).astype(BF16)
    rows = rows_ref[...]
    table = dot(rows, win[...]).astype(BF16)
    edges = meta_ref.shape[0]
    block = CHUNK
    for i in range(edges // block):
        at = slice(i * block, (i + 1) * block)
        meta = meta_ref[at, :]
        places = meta[:, 0:2].astype(F32)
        sender = (places[:, 0:1] * float(SPLIT) + places[:, 1:2]).astype(I32)
        source = lax.broadcasted_iota(I32, (block, rows.shape[0]), 1)
        pick = jnp.where(source == sender, 1.0, 0.0).astype(BF16)
        pre = dot(pick, table) + dot(meta, proj[...])
        raw = dot(silu(pre).astype(BF16), wout[...], 1, 1)
        out_ref[at, :] = normed(raw, gain_ref[...], bias_ref[1:2, :], 1).astype(BF16)


def sums_kernel(mesh_rows, keep, start_a, start_b, table_a, table_b, msg_a, msg_b, x_ref, y_ref):
    edges, _ = msg_a.shape
    key_rows = edges // LANES
    tall = y_ref.shape[1]
    parts = 2 * tall
    quarter = mesh_rows // 4
    half = quarter // 2
    lat = lax.axis_index("lat")
    low, high = lax.rem(lat, 2), lat // 2
    lon = lax.axis_index("lon")
    mine = lon * quarter
    other = (lon ^ 2) * quarter
    ready = min(key_rows, WINDOW)
    sets = ((start_a, table_a, msg_a), (start_b, table_b, msg_b))

    def sums(part, bases):
        rows = half * len(bases)
        row = lax.broadcasted_iota(I32, (rows, LANES), 0)
        node = row + (bases[0] + part * mesh_rows)
        for k in range(1, len(bases)):
            node = jnp.where(row >= k * half, row + (bases[k] - k * half + part * mesh_rows), node)

        def term(at, count, table, msg):
            pick = jnp.concatenate(
                [jnp.where(node == table[pl.ds(at + k, 1), :], 1.0, 0.0).astype(BF16) for k in range(count)], 1
            )
            return dot(pick, msg[pl.ds(pl.multiple_of(at * LANES, LANES), count * LANES), :])

        total = None
        later = []
        for start, table, msg in sets:
            begin = start[key_rows + part, 0]
            following = jnp.minimum(part + 1, parts - 1)
            end = jnp.where(part + 1 < parts, start[key_rows + following, 0], edges)
            at = jnp.minimum(begin // LANES, key_rows - ready)
            now = term(at, ready, table, msg)
            total = now if total is None else total + now
            later.append((at + ready, (end + LANES - 1) // LANES, table, msg))
        for at, end, table, msg in later:
            total = lax.fori_loop(at, end, lambda i, t, table=table, msg=msg: t + term(i, 1, table, msg), total)
        return total.astype(BF16)

    near_low = low if keep else 1 - low
    base = mine if keep else other

    @pl.loop(0, tall)
    def _(i):
        both = sums(2 * i + near_low, (base, mine + half, other + half))
        one = sums(2 * i + 1 - near_low, (base,))
        to = i ^ high
        x_ref[0 if keep else 1, to] = both[:half]
        x_ref[1 if keep else 0, to] = one
        y_ref[0, to] = both[half : 2 * half]
        y_ref[1, to] = both[2 * half :]


def node_sums(keep, tables, messages, lat_count, mesh_rows):
    tall = lat_count // 2
    edges, width = messages[0].shape
    out = jax.ShapeDtypeStruct((2, tall, mesh_rows // 8, width), BF16)
    return call(
        functools.partial(sums_kernel, mesh_rows, keep), [out, out], [SMEM] * 2 + [VMEM] * 4, 2 * edges * mesh_rows * width
    )(*tables, *tables, *messages)


def join_kernel(keep_x, got_x, got_xy, keep_y, got_y, got_yx, *outs):
    half = keep_x.shape[2]
    for j, out in enumerate(outs):
        out[:half] = (keep_x[0, j].astype(F32) + got_x[0, j].astype(F32) + got_xy[j].astype(F32)).astype(BF16)
        out[half:] = (keep_y[0, j].astype(F32) + got_y[0, j].astype(F32) + got_yx[j].astype(F32)).astype(BF16)


def node_kernel(n_base, n_agg, n_out, *refs):
    bases, refs = refs[:n_base], refs[n_base:]
    aggs, refs = refs[:n_agg], refs[n_agg:]
    bias_ref, gain_ref, w0, w1, w2, w3 = refs[:6]
    outs = refs[6 : 6 + n_out]
    base, win, wout = refs[6 + n_out :]
    width = base.shape[1]
    quarter = w0.shape[1]
    lon = lax.axis_index("lon")
    biases = []
    for j, w in enumerate((w0, w1, w2, w3)):
        win[:, j * quarter : (j + 1) * quarter] = w[0 : 2 * width, :]
        for m in range(width // quarter):
            wout[j * quarter : (j + 1) * quarter, m * quarter : (m + 1) * quarter] = w[
                2 * width + m * quarter : 2 * width + (m + 1) * quarter, :
            ]
        at = pl.ds(pl.multiple_of((lon ^ j) * quarter, quarter), quarter)
        biases.append(bias_ref[0:1, at])
        if n_base > 1:
            base[:, at] = bases[j][...]
    if n_base == 1:
        base[...] = bases[0][...]
    total = None
    for ref in aggs:
        term = ref[...] if len(ref.shape) == 2 else ref[0]
        total = term.astype(F32) if total is None else total + term.astype(F32)
    own = base[...]
    pre = dot(own, win[0:width, :]) + dot(total.astype(BF16), win[width:, :]) + jnp.concatenate(biases, 1)
    raw = dot(silu(pre).astype(BF16), wout[...])
    new = (own.astype(F32) + normed(raw, gain_ref[...], bias_ref[1:2, :], 1)).astype(BF16)
    if n_out == 1:
        outs[0][...] = new
    else:
        base[...] = new
        for j in range(n_out):
            outs[j][...] = base[:, pl.ds(pl.multiple_of((lon ^ j) * quarter, quarter), quarter)]


def node_network(bases, aggregates, biases, gain, pieces, n_out):
    rows, width = bases[0].shape[0], gain.shape[0]
    quarter = pieces[0].shape[1]
    kernel = functools.partial(node_kernel, len(bases), len(aggregates), n_out)
    scratch = [pltpu.VMEM((rows, width), BF16), pltpu.VMEM((2 * width, width), BF16), pltpu.VMEM((width, width), BF16)]
    out = jax.ShapeDtypeStruct((rows, width if n_out == 1 else quarter), BF16)
    operands = (*bases, *aggregates, biases, gain[None, :], *pieces)
    return call(
        kernel, out if n_out == 1 else [out] * n_out, [VMEM] * len(operands), 6 * rows * width * width, scratch
    )(*operands)


def lay_kernel(*refs):
    pieces, out_ref = refs[:4], refs[4]
    rows = pieces[0].shape[0]
    for j in range(4):
        out_ref[pl.ds(pl.multiple_of((lax.axis_index("lon") ^ j) * rows, rows), rows), :] = pieces[j][...]


def pick_kernel(index_ref, table_ref, *refs):
    outs, held = refs[:-1], refs[-1]
    lane = lax.broadcasted_iota(I32, (index_ref.shape[0], table_ref.shape[0]), 1)
    pick = jnp.where(lane == index_ref[...], 1.0, 0.0).astype(BF16)
    held[...] = dot(pick, table_ref[...])
    half = outs[0].shape[0]
    core = lax.rem(lax.axis_index("lon"), 2)
    for j, out in enumerate(outs):
        at = (lax.axis_index("lat") ^ j) * (2 * half)
        rows = held[pl.ds(pl.multiple_of(at, 2 * half), 2 * half), :]
        out[...] = jnp.where(core == 0, rows[:half], rows[half:]).astype(BF16)


def pack_kernel(*refs):
    out_ref = refs[-1]
    out_ref[...] = jnp.concatenate([ref[...].astype(F32) for ref in refs[:-1]], 0).astype(BF16)


def near_kernel(edge_hbm, mid_ref, ends_ref, bias_ref, w0, w1, w2, w3, out_ref, win, edge_ref, sem):
    block = CHUNK
    edges, width = edge_ref.shape
    loads = []
    for i in range(edges // block):
        at = pl.ds(i * block, block)
        loads.append(pltpu.make_async_copy(edge_hbm.at[at, :], edge_ref.at[at, :], sem.at[i]))
        loads[-1].start()
    quarter = w0.shape[1]
    lon = lax.axis_index("lon")
    biases = []
    for j, w in enumerate((w0, w1, w2, w3)):
        win[:, j * quarter : (j + 1) * quarter] = w[0 : 3 * width, :]
        at = pl.ds(pl.multiple_of((lon ^ j) * quarter, quarter), quarter)
        biases.append(bias_ref[0:1, at])
    bias = jnp.concatenate(biases, 1)
    rows = mid_ref.shape[0]
    sent = dot(mid_ref[...], win[width : 2 * width, :]).astype(BF16)
    got = dot(mid_ref[...], win[2 * width :, :]).astype(BF16)
    for i in range(edges // block):
        at = slice(i * block, (i + 1) * block)
        lane = lax.broadcasted_iota(I32, (block, rows), 1)
        pick_s = jnp.where(lane == ends_ref[at, 0:1], 1.0, 0.0).astype(BF16)
        pick_r = jnp.where(lane == ends_ref[at, 1:2], 1.0, 0.0).astype(BF16)
        pre = dot(pick_s, sent) + dot(pick_r, got) + bias
        loads[i].wait()
        out_ref[at, :] = pre + dot(edge_ref[at, :], win[0:width, :])


def far_kernel(halo_cap, edge_hbm, pre_ref, halo_a, halo_b, ends_ref, receiver_ref, bias_ref, gain_ref, w0, w1, w2, w3, new_ref, away_ref, keep_ref, pass_ref, total, win, wout, edge_ref, sem):
    load = pltpu.make_async_copy(edge_hbm, edge_ref, sem)
    load.start()
    width = halo_a.shape[1]
    quarter = w0.shape[1]
    lon = lax.axis_index("lon")
    for j, w in enumerate((w0, w1, w2, w3)):
        win[:, j * quarter : (j + 1) * quarter] = w[width : 2 * width, :]
        wout[:, j * quarter : (j + 1) * quarter] = w[3 * width : 4 * width, :]
    rows = halo_a.shape[0]
    mesh_rows = total.shape[0]
    sent = [dot(h[...], win[...]).astype(BF16) for h in (halo_a, halo_b)]
    half = halo_cap // 2
    lane = lax.broadcasted_iota(I32, (1, rows), 1)
    core = lax.rem(lon, 2)
    source = (lane // half) ^ lax.axis_index("lat")
    names = [mesh_rows + source * halo_cap + lane % half + c * half for c in (core, 1 - core)]
    edges = edge_ref.shape[0]
    block = 256
    for i in range(edges // block):
        at = slice(i * block, (i + 1) * block)
        pre = pre_ref[at, :]
        for name, rows_in in zip(names, sent):
            pick = jnp.where(name == ends_ref[at, 0:1], 1.0, 0.0).astype(BF16)
            pre = pre + dot(pick, rows_in)
        if i == 0:
            load.wait()
        raw = dot(silu(pre).astype(BF16), wout[...], 1, 1)
        new_ref[at, :] = (edge_ref[at, :].astype(F32) + normed(raw, gain_ref[...], bias_ref[1:2, :], 1)).astype(BF16)
    node = lax.broadcasted_iota(I32, (mesh_rows, edges), 0)
    onto = jnp.where(node == receiver_ref[...], 1.0, 0.0).astype(BF16)
    total[...] = dot(onto, new_ref[...]).astype(BF16)
    rows = keep_ref.shape[0]

    def part(flip):
        return total[pl.ds(pl.multiple_of((lon ^ flip) * rows, rows), rows), :]

    away_ref[0] = part(1)
    away_ref[1] = part(3)
    keep_ref[...] = part(0)
    pass_ref[...] = part(2)


def plus(*values):
    total = values[0].astype(F32)
    for v in values[1:]:
        total = total + v.astype(F32)
    return total.astype(BF16)


def local(
    grid_latent,
    grid_feat,
    grid_sender,
    grid_owner,
    grid_node,
    mesh_latent,
    mesh_edge,
    halo_send,
    mesh_sender,
    mesh_receiver,
    enc_edge_in,
    enc_feat_proj,
    enc_edge_out,
    enc_edge_bias,
    enc_edge_gain,
    enc_node_in,
    enc_node_out,
    enc_node_bias,
    enc_node_gain,
    proc_edge_in,
    proc_edge_out,
    proc_edge_bias,
    proc_edge_gain,
    proc_node_in,
    proc_node_out,
    proc_node_bias,
    proc_node_gain,
):
    lat_count = lax.axis_size("lat")
    width = grid_latent.shape[1]
    quarter = mesh_latent.shape[1]
    mesh_rows = mesh_latent.shape[0]
    node_rows = mesh_rows // 4
    edges = grid_sender.shape[0]
    local_edges = mesh_edge.shape[0]
    halo_cap = halo_send.shape[1]
    listed = halo_send.size

    def like(rows, columns, kind=BF16):
        return jax.ShapeDtypeStruct((rows, columns), kind)

    def hop(values, axis, flip):
        size = lax.axis_size(axis)
        return lax.ppermute(values, axis, [(i, i ^ flip) for i in range(size)])

    def spread(shard):
        across = hop(shard, "lon", 2)
        return (shard, hop(shard, "lon", 1), across, hop(across, "lon", 1))

    enc_in = spread(enc_edge_in)
    enc_out = spread(enc_edge_out)
    small = (grid_owner.reshape(1, edges), grid_sender[None, :], grid_node[None, :], grid_feat)
    small = small + (halo_send, mesh_sender[None, :], mesh_receiver[None, :])
    deep = 2 * width + 4 * enc_node_out.shape[0]
    copies = 4 + 2 * (1 + width // quarter) + 2
    table, meta, ends, asked, *rest = call(
        functools.partial(open_kernel, lat_count, mesh_rows),
        [
            like(edges // LANES + lat_count, LANES, I32),
            like(edges, META),
            like(local_edges, 8, I32),
            like(listed, 1, I32),
        ]
        + [like(node_rows, quarter)] * 4
        + [like(deep, quarter), like(4 * width, quarter), like(deep, quarter)],
        [HBM] * 14,
        2 * META * edges * edges * 8,
        [pltpu.VMEM(v.shape, v.dtype) for v in small]
        + [pltpu.SemaphoreType.DMA((len(small),)), pltpu.SemaphoreType.DMA((copies,))],
        FULL,
    )(*small, mesh_latent, enc_node_in, enc_node_out, proc_edge_in, proc_edge_out, proc_node_in, proc_node_out)
    bases = tuple(rest[j] if j == 0 else hop(rest[j], "lon", j) for j in range(4))
    node_pieces = spread(rest[4])
    edge_pieces = spread(rest[5])
    last_pieces = spread(rest[6])

    tables = (table, hop(table, "lon", 1))
    message = call(
        functools.partial(message_kernel, grid_feat.shape[0]),
        like(edges, width),
        [VMEM] * 13,
        4 * edges * width * width,
        [pltpu.VMEM((width, width), BF16), pltpu.VMEM((width, width), BF16), pltpu.VMEM((META, width), BF16)],
    )(grid_latent, meta, enc_feat_proj, enc_edge_bias, enc_edge_gain[None, :], *enc_in, *enc_out)
    messages = (message, hop(message, "lon", 1))

    tall = lat_count // 2
    send_x, send_y = node_sums(False, tables, messages, lat_count, mesh_rows)
    got_x = hop(send_x, "lon", 2)
    got_y = hop(send_y, "lat", 1)
    keep_x, keep_y = node_sums(True, tables, messages, lat_count, mesh_rows)
    got_xy = hop(plus(keep_x[1], got_x[1]), "lat", 1)
    got_yx = hop(plus(keep_y[1], got_y[1]), "lon", 2)
    joined = call(join_kernel, [like(node_rows, width)] * tall, [VMEM] * 6, 1 << 20)(
        keep_x, got_x, got_xy, keep_y, got_y, got_yx
    )
    partials = tuple(joined[j] if j == 0 else hop(joined[j], "lat", 2 * j) for j in range(tall))

    mid = node_network(bases, partials, enc_node_bias, enc_node_gain, node_pieces, 1)
    mid_all = lax.all_gather(mid, "lon", axis=0, tiled=True)

    half_cap = halo_cap // 2
    picked = call(
        pick_kernel,
        [like(half_cap, width)] * lat_count,
        [VMEM] * 2,
        2 * listed * mesh_rows * width,
        [pltpu.VMEM((listed, width), F32)],
    )(asked, mid_all)
    arrived = [picked[j] if j == 0 else hop(picked[j], "lat", j) for j in range(lat_count)]
    near = call(
        near_kernel,
        like(local_edges, width, F32),
        [HBM] + [VMEM] * 7,
        2 * local_edges * width * (width + 2 * mesh_rows),
        [
            pltpu.VMEM((3 * width, width), BF16),
            pltpu.VMEM((local_edges, width), BF16),
            pltpu.SemaphoreType.DMA((local_edges // CHUNK,)),
        ],
    )(mesh_edge, mid_all, ends, proc_edge_bias, *edge_pieces)
    packed = call(pack_kernel, like(listed // 2, width), [VMEM] * lat_count, 1 << 20)(*arrived)
    halves = (packed, hop(packed, "lon", 1))

    edge_update, away, kept, passed = call(
        functools.partial(far_kernel, halo_cap),
        [
            like(local_edges, width),
            jax.ShapeDtypeStruct((2, node_rows, width), BF16),
            like(node_rows, width),
            like(node_rows, width),
        ],
        [HBM] + [VMEM] * 11,
        2 * local_edges * width * (width + listed + mesh_rows),
        [
            pltpu.VMEM((mesh_rows, width), BF16),
            pltpu.VMEM((width, width), BF16),
            pltpu.VMEM((width, width), BF16),
            pltpu.VMEM((local_edges, width), BF16),
            pltpu.SemaphoreType.DMA,
        ],
    )(mesh_edge, near, *halves, ends, mesh_receiver[None, :], proc_edge_bias, proc_edge_gain[None, :], *edge_pieces)

    came = hop(away, "lon", 1)
    got = hop(plus(passed, came[1]), "lon", 2)
    new = node_network((mid,), (kept, came, got), proc_node_bias, proc_node_gain, last_pieces, 4)
    mesh_update = call(lay_kernel, like(mesh_rows, quarter), [VMEM] * 4, 1 << 20)(
        new[0], *[hop(new[j], "lon", j) for j in (1, 2, 3)]
    )
    return (mesh_update, edge_update)


def solution(mesh):
    both = ("lat", "lon")
    placed = (
        P(both, None),
        P(None, both),
        P(both),
        P(both, None),
        P(both),
        P("lat", "lon"),
        P(both, None),
        P("lat", None),
        P(both),
        P(both),
        P(None, "lon"),
        P(),
        P(None, "lon"),
        P(),
        P(),
        P(None, "lon"),
        P("lon", None),
        P(),
        P(),
        P(None, "lon"),
        P(None, "lon"),
        P(),
        P(),
        P(None, "lon"),
        P("lon", None),
        P(),
        P(),
    )

    return jax.shard_map(
        local,
        mesh=mesh,
        in_specs=placed,
        out_specs=(P("lat", "lon"), P(both, None)),
        check_vma=False,
    )
```

```python
import functools
import jax
import jax.numpy as jnp
from jax import lax
from jax.experimental import pallas as pl
from jax.experimental.pallas import tpu as pltpu
from jax.sharding import PartitionSpec as P


F32 = jnp.float32
BF16 = jnp.bfloat16
I32 = jnp.int32
SPLIT = 32
CHUNK = 256
LANES = 128
GRANT = 16 << 20
FULL = 59 << 20
META = 16

VMEM = pl.BlockSpec(memory_space=pltpu.VMEM)
SMEM = pl.BlockSpec(memory_space=pltpu.SMEM)
HBM = pl.BlockSpec(memory_space=pltpu.HBM)


def dot(a, b, ca=1, cb=0):
    return lax.dot_general(a, b, (((ca,), (cb,)), ((), ())), preferred_element_type=F32)


def turns(count):
    flips = sorted(range(count), key=lambda f: (-(f % 2 + f // 2), -f))
    shares = [f for k, f in enumerate(flips) if k % 4 in (0, 3)], [f for k, f in enumerate(flips) if k % 4 in (1, 2)]
    return list(zip(*sorted(shares, key=lambda share: share[-1])))


def cost(flops, nbytes):
    return pl.CostEstimate(flops=int(flops), bytes_accessed=int(nbytes), transcendentals=0)


def call(kernel, out_shape, specs, flops, scratch=(), grant=GRANT):
    many = isinstance(out_shape, list)
    return pl.pallas_call(
        kernel,
        out_shape=out_shape,
        in_specs=specs,
        out_specs=[VMEM] * len(out_shape) if many else VMEM,
        scratch_shapes=list(scratch),
        cost_estimate=cost(flops, 4 << 20),
        compiler_params=pltpu.CompilerParams(vmem_limit_bytes=grant),
    )


def silu(t):
    return 0.5 * t * (1.0 + jnp.tanh(0.5 * t))


def normed(raw, gain, offset, axis):
    width = raw.shape[axis]
    average = jnp.sum(raw, axis=axis, keepdims=True) * (1.0 / width)
    centred = raw - average
    spread = jnp.sum(centred * centred, axis=axis, keepdims=True) * (1.0 / width)
    return centred * lax.rsqrt(spread + 1e-05) * gain + offset


def columns_of(rows):
    height, width = rows.shape
    rows = rows.astype(F32)
    if height % 8:
        rows = jnp.concatenate([rows, jnp.zeros((8 - height % 8, width), F32)], 0)
    if width % LANES:
        rows = jnp.concatenate([rows, jnp.zeros((rows.shape[0], LANES - width % LANES), F32)], 1)
    return jnp.transpose(rows)


def open_kernel(
    lat_count,
    mesh_rows,
    owner_hbm,
    sender_hbm,
    node_hbm,
    feat_hbm,
    halo_hbm,
    from_hbm,
    to_hbm,
    latent,
    table_ref,
    meta_ref,
    ends_ref,
    asked_ref,
    base0,
    base1,
    base2,
    base3,
    owner_ref,
    sender_ref,
    node_ref,
    feat_ref,
    halo_ref,
    from_ref,
    to_ref,
    first_sem,
    sem,
):
    lon = lax.axis_index("lon")
    rows = base0.shape[0]
    inputs = (owner_hbm, sender_hbm, node_hbm, feat_hbm, halo_hbm, from_hbm, to_hbm)
    held = (owner_ref, sender_ref, node_ref, feat_ref, halo_ref, from_ref, to_ref)
    early = [pltpu.make_async_copy(a, b, first_sem.at[k]) for k, (a, b) in enumerate(zip(inputs, held))]
    late = []

    def bring(source, target):
        late.append(pltpu.make_async_copy(source, target, sem.at[len(late)]))

    for j, base in enumerate((base0, base1, base2, base3)):
        bring(latent.at[pl.ds(pl.multiple_of((lon ^ j) * rows, rows), rows), :], base)
    for copy in early + late:
        copy.start()
    for copy in early:
        copy.wait()
    ends_ref[...] = columns_of(jnp.concatenate([from_ref[...].astype(F32), to_ref[...].astype(F32)], 0)).astype(I32)
    asked = columns_of(halo_ref[...]).astype(I32)
    cap = halo_ref.shape[1]
    for p in range(lat_count):
        asked_ref[p * cap : (p + 1) * cap, :] = asked[0:cap, p : p + 1]
    edges = owner_ref.shape[1]
    owner = owner_ref[...]
    parts = lax.broadcasted_iota(I32, (lat_count, edges), 0)
    hits = jnp.where(parts == owner, 1.0, 0.0)
    lane = lax.broadcasted_iota(I32, (lat_count, edges), 1)
    count = hits
    step = 1
    while step < edges:
        count = count + jnp.where(lane >= step, pltpu.roll(count, step, 1), 0.0)
        step *= 2
    first = jnp.sum(jnp.where(owner < parts, 1.0, 0.0), axis=1, keepdims=True)
    place = jnp.sum(hits * (first + count - hits), axis=0, keepdims=True).astype(I32)
    key_rows = edges // LANES
    table_ref[key_rows:, :] = jnp.broadcast_to(first, (lat_count, LANES)).astype(I32)
    sender = sender_ref[...]
    node = node_ref[...]
    digits = [sender // SPLIT, sender % SPLIT, node // SPLIT, node % SPLIT, owner]
    rows = [d.astype(F32) for d in digits] + [feat_ref[...].astype(F32)]
    used = len(digits) + feat_ref.shape[0]
    meta = jnp.concatenate(rows + [jnp.ones((META - used, edges), F32)], 0).astype(BF16)
    for i in range(edges // CHUNK):
        spot = lax.broadcasted_iota(I32, (CHUNK, edges), 0) + i * CHUNK
        perm = jnp.where(spot == place, 1.0, 0.0).astype(BF16)
        moved = dot(meta, perm, 1, 1)
        meta_ref[:, i * CHUNK : (i + 1) * CHUNK] = moved.astype(BF16)
        key = moved[4:5] * float(mesh_rows) + moved[2:3] * float(SPLIT) + moved[3:4]
        for k in range(CHUNK // LANES):
            row = i * (CHUNK // LANES) + k
            table_ref[row : row + 1, :] = key[:, k * LANES : (k + 1) * LANES].astype(I32)
    for copy in late:
        copy.wait()


def message_kernel(n_feat, rows_ref, meta_ref, proj_ref, bias_ref, gain_ref, w0, w1, w2, w3, v0, v1, v2, v3, out_ref, win, wout, proj):
    quarter = w0.shape[1]
    lon = lax.axis_index("lon")
    for j, (w, v) in enumerate(((w0, v0), (w1, v1), (w2, v2), (w3, v3))):
        win[:, j * quarter : (j + 1) * quarter] = w[...]
        wout[:, j * quarter : (j + 1) * quarter] = v[...]
        at = pl.ds(pl.multiple_of((lon ^ j) * quarter, quarter), quarter)
        bias = bias_ref[0:1, at]
        high = bias.astype(BF16).astype(F32)
        mid = (bias - high).astype(BF16).astype(F32)
        low = bias - high - mid
        used = META - 5 - n_feat
        proj[:, j * quarter : (j + 1) * quarter] = jnp.concatenate(
            [jnp.zeros((5, quarter), F32), proj_ref[:, at].astype(F32), high, mid, low, jnp.zeros((used - 3, quarter), F32)], 0
        ).astype(BF16)
    rows = rows_ref[...]
    table = dot(rows, win[...]).astype(BF16)
    edges = meta_ref.shape[1]
    block = CHUNK
    for i in range(edges // block):
        at = slice(i * block, (i + 1) * block)
        places = jnp.transpose(meta_ref[:, at].astype(F32))
        meta = places.astype(BF16)
        sender = (places[:, 0:1] * float(SPLIT) + places[:, 1:2]).astype(I32)
        source = lax.broadcasted_iota(I32, (block, rows.shape[0]), 1)
        pick = jnp.where(source == sender, 1.0, 0.0).astype(BF16)
        pre = dot(pick, table) + dot(meta, proj[...])
        raw = dot(silu(pre).astype(BF16), wout[...], 1, 1)
        out_ref[at, :] = normed(raw, gain_ref[...], bias_ref[1:2, :], 1).astype(BF16)


def sums_kernel(mesh_rows, cap, keep, start_a, start_b, table_a, table_b, msg_a, msg_b, x_ref, y_ref):
    edges, _ = msg_a.shape
    key_rows = edges // LANES
    tall = y_ref.shape[1]
    quarter = mesh_rows // 4
    half = quarter // 2
    lat = lax.axis_index("lat")
    low, high = lax.rem(lat, 2), lat // 2
    lon = lax.axis_index("lon")
    mine = lon * quarter
    other = (lon ^ 2) * quarter
    ready = min(key_rows, (cap + 2 * LANES - 2) // LANES)
    sets = ((start_a, table_a, msg_a), (start_b, table_b, msg_b))

    def sums(part, bases):
        rows = half * len(bases)
        row = lax.broadcasted_iota(I32, (rows, LANES), 0)
        node = row + (bases[0] + part * mesh_rows)
        for k in range(1, len(bases)):
            node = jnp.where(row >= k * half, row + (bases[k] - k * half + part * mesh_rows), node)

        total = None
        for start, table, msg in sets:
            at = jnp.minimum(start[key_rows + part, 0] // LANES, key_rows - ready)
            pick = jnp.concatenate(
                [jnp.where(node == table[pl.ds(at + k, 1), :], 1.0, 0.0).astype(BF16) for k in range(ready)], 1
            )
            term = dot(pick, msg[pl.ds(pl.multiple_of(at * LANES, LANES), ready * LANES), :])
            total = term if total is None else total + term
        return total.astype(BF16)

    near_low = low if keep else 1 - low
    base = mine if keep else other

    @pl.loop(0, tall, unroll=2)
    def _(i):
        both = sums(2 * i + near_low, (base, mine + half, other + half))
        one = sums(2 * i + 1 - near_low, (base,))
        to = i ^ high
        x_ref[0 if keep else 1, to] = both[:half]
        x_ref[1 if keep else 0, to] = one
        y_ref[0, to] = both[half : 2 * half]
        y_ref[1, to] = both[2 * half :]


def node_sums(keep, tables, messages, lat_count, mesh_rows):
    tall = lat_count // 2
    edges, width = messages[0].shape
    out = jax.ShapeDtypeStruct((2, tall, mesh_rows // 8, width), BF16)
    return call(
        functools.partial(sums_kernel, mesh_rows, 2 * edges // lat_count, keep), [out, out], [SMEM] * 2 + [VMEM] * 4, 2 * edges * mesh_rows * width
    )(*tables, *tables, *messages)


def join_kernel(keep_x, got_x, got_xy, keep_y, got_y, got_yx, *outs):
    half = keep_x.shape[2]
    for j, out in enumerate(outs):
        out[:half] = (keep_x[0, j].astype(F32) + got_x[0, j].astype(F32) + got_xy[j].astype(F32)).astype(BF16)
        out[half:] = (keep_y[0, j].astype(F32) + got_y[0, j].astype(F32) + got_yx[j].astype(F32)).astype(BF16)


def node_kernel(n_base, n_agg, n_out, *refs):
    bases, refs = refs[:n_base], refs[n_base:]
    aggs, refs = refs[:n_agg], refs[n_agg:]
    bias_ref, gain_ref = refs[:2]
    weights = refs[2:10]
    outs = refs[10 : 10 + n_out]
    base, win, wout = refs[10 + n_out :]
    width = base.shape[1]
    quarter = weights[0].shape[1]
    lon = lax.axis_index("lon")
    biases = []
    for j in range(4):
        win[:, j * quarter : (j + 1) * quarter] = weights[j][...]
        wout[j * quarter : (j + 1) * quarter, :] = weights[4 + j][...]
        at = pl.ds(pl.multiple_of((lon ^ j) * quarter, quarter), quarter)
        biases.append(bias_ref[0:1, at])
        if n_base > 1:
            base[:, at] = bases[j][...]
    if n_base == 1:
        base[...] = bases[0][...]
    total = None
    for ref in aggs:
        term = ref[...] if len(ref.shape) == 2 else ref[0]
        total = term.astype(F32) if total is None else total + term.astype(F32)
    own = base[...]
    pre = dot(own, win[0:width, :]) + dot(total.astype(BF16), win[width:, :]) + jnp.concatenate(biases, 1)
    raw = dot(silu(pre).astype(BF16), wout[...])
    new = (own.astype(F32) + normed(raw, gain_ref[...], bias_ref[1:2, :], 1)).astype(BF16)
    if n_out == 1:
        outs[0][...] = new
    else:
        base[...] = new
        for j in range(n_out):
            outs[j][...] = base[:, pl.ds(pl.multiple_of((lon ^ j) * quarter, quarter), quarter)]


def node_network(bases, aggregates, biases, gain, pieces, n_out):
    rows, width = bases[0].shape[0], gain.shape[0]
    quarter = pieces[0].shape[1]
    kernel = functools.partial(node_kernel, len(bases), len(aggregates), n_out)
    scratch = [pltpu.VMEM((rows, width), BF16), pltpu.VMEM((2 * width, width), BF16), pltpu.VMEM((width, width), BF16)]
    out = jax.ShapeDtypeStruct((rows, width if n_out == 1 else quarter), BF16)
    operands = (*bases, *aggregates, biases, gain[None, :], *pieces)
    return call(
        kernel, out if n_out == 1 else [out] * n_out, [VMEM] * len(operands), 6 * rows * width * width, scratch
    )(*operands)


def lay_kernel(*refs):
    pieces, out_ref = refs[:4], refs[4]
    rows = pieces[0].shape[0]
    for j in range(4):
        out_ref[pl.ds(pl.multiple_of((lax.axis_index("lon") ^ j) * rows, rows), rows), :] = pieces[j][...]


def pick_kernel(index_ref, table_ref, *refs):
    outs, held = refs[:-1], refs[-1]
    lane = lax.broadcasted_iota(I32, (index_ref.shape[0], table_ref.shape[0]), 1)
    pick = jnp.where(lane == index_ref[...], 1.0, 0.0).astype(BF16)
    held[...] = dot(pick, table_ref[...])
    cap = outs[0].shape[0]
    core = lax.rem(lax.axis_index("lon"), 2)
    for out, (flip0, flip1) in zip(outs, turns(2 * len(outs))):
        at = (lax.axis_index("lat") ^ jnp.where(core == 0, flip0, flip1)) * cap
        out[...] = held[pl.ds(pl.multiple_of(at, cap), cap), :].astype(BF16)


def pack_kernel(own_ref, *refs):
    out_ref = refs[-1]
    core = lax.rem(lax.axis_index("lon"), 2)
    last = jnp.where(core == 0, own_ref[...].astype(F32), refs[-2][...].astype(F32))
    out_ref[...] = jnp.concatenate([ref[...].astype(F32) for ref in refs[:-2]] + [last], 0).astype(BF16)


def near_kernel(edge_hbm, mid_ref, ends_ref, bias_ref, w0, w1, w2, w3, out_ref, win, edge_ref, sem):
    block = CHUNK
    edges, width = edge_ref.shape
    loads = []
    for i in range(edges // block):
        at = pl.ds(i * block, block)
        loads.append(pltpu.make_async_copy(edge_hbm.at[at, :], edge_ref.at[at, :], sem.at[i]))
        loads[-1].start()
    quarter = w0.shape[1]
    lon = lax.axis_index("lon")
    biases = []
    for j, w in enumerate((w0, w1, w2, w3)):
        win[:, j * quarter : (j + 1) * quarter] = w[...]
        at = pl.ds(pl.multiple_of((lon ^ j) * quarter, quarter), quarter)
        biases.append(bias_ref[0:1, at])
    bias = jnp.concatenate(biases, 1)
    rows = mid_ref.shape[0]
    sent = dot(mid_ref[...], win[width : 2 * width, :]).astype(BF16)
    got = dot(mid_ref[...], win[2 * width :, :]).astype(BF16)
    for i in range(edges // block):
        at = slice(i * block, (i + 1) * block)
        lane = lax.broadcasted_iota(I32, (block, rows), 1)
        pick_s = jnp.where(lane == ends_ref[at, 0:1], 1.0, 0.0).astype(BF16)
        pick_r = jnp.where(lane == ends_ref[at, 1:2], 1.0, 0.0).astype(BF16)
        pre = dot(pick_s, sent) + dot(pick_r, got) + bias
        loads[i].wait()
        out_ref[at, :] = pre + dot(edge_ref[at, :], win[0:width, :])


def far_kernel(halo_cap, edge_hbm, pre_ref, halo_a, halo_b, ends_ref, receiver_ref, bias_ref, gain_ref, w0, w1, w2, w3, v0, v1, v2, v3, new_ref, away_ref, keep_ref, pass_ref, total, win, wout, edge_ref, sem):
    load = pltpu.make_async_copy(edge_hbm, edge_ref, sem)
    load.start()
    width = halo_a.shape[1]
    quarter = w0.shape[1]
    lon = lax.axis_index("lon")
    for j, (w, v) in enumerate(((w0, v0), (w1, v1), (w2, v2), (w3, v3))):
        win[:, j * quarter : (j + 1) * quarter] = w[width : 2 * width, :]
        wout[:, j * quarter : (j + 1) * quarter] = v[...]
    rows = halo_a.shape[0]
    mesh_rows = total.shape[0]
    sent = [dot(h[...], win[...]).astype(BF16) for h in (halo_a, halo_b)]
    lane = lax.broadcasted_iota(I32, (1, rows), 1)
    core = lax.rem(lon, 2)
    lat = lax.axis_index("lat")
    flips = [jnp.zeros_like(lane), jnp.zeros_like(lane)]
    for j, pair in enumerate(turns(2 * (rows // halo_cap))):
        flips = [jnp.where(lane // halo_cap == j, flip, before) for flip, before in zip(pair, flips)]
    flips = [jnp.where(core == 0, a, b) for a, b in (flips, flips[::-1])]
    names = [mesh_rows + (lat ^ flip) * halo_cap + lane % halo_cap for flip in flips]
    edges = edge_ref.shape[0]
    block = 256
    for i in range(edges // block):
        at = slice(i * block, (i + 1) * block)
        pre = pre_ref[at, :]
        for name, rows_in in zip(names, sent):
            pick = jnp.where(name == ends_ref[at, 0:1], 1.0, 0.0).astype(BF16)
            pre = pre + dot(pick, rows_in)
        if i == 0:
            load.wait()
        raw = dot(silu(pre).astype(BF16), wout[...], 1, 1)
        new_ref[at, :] = (edge_ref[at, :].astype(F32) + normed(raw, gain_ref[...], bias_ref[1:2, :], 1)).astype(BF16)
    node = lax.broadcasted_iota(I32, (mesh_rows, edges), 0)
    onto = jnp.where(node == receiver_ref[...], 1.0, 0.0).astype(BF16)
    total[...] = dot(onto, new_ref[...]).astype(BF16)
    rows = keep_ref.shape[0]

    def part(flip):
        return total[pl.ds(pl.multiple_of((lon ^ flip) * rows, rows), rows), :]

    away_ref[0] = part(1)
    away_ref[1] = part(3)
    keep_ref[...] = part(0)
    pass_ref[...] = part(2)


def plus(*values):
    total = values[0].astype(F32)
    for v in values[1:]:
        total = total + v.astype(F32)
    return total.astype(BF16)


def local(
    grid_latent,
    grid_feat,
    grid_sender,
    grid_owner,
    grid_node,
    mesh_latent,
    mesh_edge,
    halo_send,
    mesh_sender,
    mesh_receiver,
    enc_edge_in,
    enc_feat_proj,
    enc_edge_out,
    enc_edge_bias,
    enc_edge_gain,
    enc_node_in,
    enc_node_out,
    enc_node_bias,
    enc_node_gain,
    proc_edge_in,
    proc_edge_out,
    proc_edge_bias,
    proc_edge_gain,
    proc_node_in,
    proc_node_out,
    proc_node_bias,
    proc_node_gain,
):
    lat_count = lax.axis_size("lat")
    width = grid_latent.shape[1]
    quarter = mesh_latent.shape[1]
    mesh_rows = mesh_latent.shape[0]
    node_rows = mesh_rows // 4
    edges = grid_sender.shape[0]
    local_edges = mesh_edge.shape[0]
    halo_cap = halo_send.shape[1]
    listed = halo_send.size

    def like(rows, columns, kind=BF16):
        return jax.ShapeDtypeStruct((rows, columns), kind)

    def hop(values, axis, flip):
        size = lax.axis_size(axis)
        return lax.ppermute(values, axis, [(i, i ^ flip) for i in range(size)])

    def spread(shard):
        across = hop(shard, "lon", 2)
        return (shard, hop(shard, "lon", 1), across, hop(across, "lon", 1))

    enc_in = spread(enc_edge_in)
    enc_out = spread(enc_edge_out)
    small = (grid_owner.reshape(1, edges), grid_sender[None, :], grid_node[None, :], grid_feat)
    small = small + (halo_send, mesh_sender[None, :], mesh_receiver[None, :])
    table, meta, ends, asked, *rest = call(
        functools.partial(open_kernel, lat_count, mesh_rows),
        [
            like(edges // LANES + lat_count, LANES, I32),
            like(META, edges),
            like(local_edges, 8, I32),
            like(listed, 1, I32),
        ]
        + [like(node_rows, quarter)] * 4,
        [HBM] * 8,
        2 * META * edges * edges * 8,
        [pltpu.VMEM(v.shape, v.dtype) for v in small]
        + [pltpu.SemaphoreType.DMA((len(small),)), pltpu.SemaphoreType.DMA((4,))],
        FULL,
    )(*small, mesh_latent)
    bases = tuple(rest[j] if j == 0 else hop(rest[j], "lon", j) for j in range(4))
    node_pieces = spread(enc_node_in) + spread(enc_node_out)
    edge_in = spread(proc_edge_in)
    edge_out = spread(proc_edge_out)
    last_pieces = spread(proc_node_in) + spread(proc_node_out)

    tables = (table, hop(table, "lon", 1))
    message = call(
        functools.partial(message_kernel, grid_feat.shape[0]),
        like(edges, width),
        [VMEM] * 13,
        4 * edges * width * width,
        [pltpu.VMEM((width, width), BF16), pltpu.VMEM((width, width), BF16), pltpu.VMEM((META, width), BF16)],
    )(grid_latent, meta, enc_feat_proj, enc_edge_bias, enc_edge_gain[None, :], *enc_in, *enc_out)
    messages = (message, hop(message, "lon", 1))

    tall = lat_count // 2
    send_x, send_y = node_sums(False, tables, messages, lat_count, mesh_rows)
    got_x = hop(send_x, "lon", 2)
    got_y = hop(send_y, "lat", 1)
    keep_x, keep_y = node_sums(True, tables, messages, lat_count, mesh_rows)
    got_xy = hop(plus(keep_x[1], got_x[1]), "lat", 1)
    got_yx = hop(plus(keep_y[1], got_y[1]), "lon", 2)
    joined = call(join_kernel, [like(node_rows, width)] * tall, [VMEM] * 6, 1 << 20)(
        keep_x, got_x, got_xy, keep_y, got_y, got_yx
    )
    far_first = sorted(range(1, tall), key=lambda j: (j < tall // 2, j))
    partials = (joined[0], *[hop(joined[j], "lat", 2 * j) for j in far_first])

    mid = node_network(bases, partials, enc_node_bias, enc_node_gain, node_pieces, 1)
    mid_all = lax.all_gather(mid, "lon", axis=0, tiled=True)

    picked = call(
        pick_kernel,
        [like(halo_cap, width)] * tall,
        [VMEM] * 2,
        2 * listed * mesh_rows * width,
        [pltpu.VMEM((listed, width), F32)],
    )(asked, mid_all)

    def halo_hop(j, flips):
        pairs = []
        for i in range(lat_count):
            for l in range(4):
                to = i ^ flips[l % 2]
                if to != i:
                    pairs.append((i * 4 + l, to * 4 + l))
        return lax.ppermute(picked[j], ("lat", "lon"), pairs)

    arrived = [halo_hop(j, flips) for j, flips in enumerate(turns(lat_count))]
    near = call(
        near_kernel,
        like(local_edges, width, F32),
        [HBM] + [VMEM] * 7,
        2 * local_edges * width * (width + 2 * mesh_rows),
        [
            pltpu.VMEM((3 * width, width), BF16),
            pltpu.VMEM((local_edges, width), BF16),
            pltpu.SemaphoreType.DMA((local_edges // CHUNK,)),
        ],
    )(mesh_edge, mid_all, ends, proc_edge_bias, *edge_in)
    packed = call(pack_kernel, like(listed // 2, width), [VMEM] * (tall + 1), 1 << 20)(picked[-1], *arrived)
    halves = (packed, hop(packed, "lon", 1))

    edge_update, away, kept, passed = call(
        functools.partial(far_kernel, halo_cap),
        [
            like(local_edges, width),
            jax.ShapeDtypeStruct((2, node_rows, width), BF16),
            like(node_rows, width),
            like(node_rows, width),
        ],
        [HBM] + [VMEM] * 15,
        2 * local_edges * width * (width + listed + mesh_rows),
        [
            pltpu.VMEM((mesh_rows, width), BF16),
            pltpu.VMEM((width, width), BF16),
            pltpu.VMEM((width, width), BF16),
            pltpu.VMEM((local_edges, width), BF16),
            pltpu.SemaphoreType.DMA,
        ],
    )(mesh_edge, near, *halves, ends, mesh_receiver[None, :], proc_edge_bias, proc_edge_gain[None, :], *edge_in, *edge_out)

    came = hop(away, "lon", 1)
    got = hop(plus(passed, came[1]), "lon", 2)
    new = node_network((mid,), (kept, came, got), proc_node_bias, proc_node_gain, last_pieces, 4)
    mesh_update = call(lay_kernel, like(mesh_rows, quarter), [VMEM] * 4, 1 << 20)(
        new[0], *[hop(new[j], "lon", j) for j in (1, 2, 3)]
    )
    return (mesh_update, edge_update)


def solution(mesh):
    both = ("lat", "lon")
    placed = (
        P(both, None),
        P(None, both),
        P(both),
        P(both, None),
        P(both),
        P("lat", "lon"),
        P(both, None),
        P("lat", None),
        P(both),
        P(both),
        P(None, "lon"),
        P(),
        P(None, "lon"),
        P(),
        P(),
        P(None, "lon"),
        P("lon", None),
        P(),
        P(),
        P(None, "lon"),
        P(None, "lon"),
        P(),
        P(),
        P(None, "lon"),
        P("lon", None),
        P(),
        P(),
    )

    return jax.shard_map(
        local,
        mesh=mesh,
        in_specs=placed,
        out_specs=(P("lat", "lon"), P(both, None)),
        check_vma=False,
    )
```

```python
import functools
import jax
import jax.numpy as jnp
from jax import lax
from jax.experimental import pallas as pl
from jax.experimental.pallas import tpu as pltpu
from jax.sharding import PartitionSpec as P


F32 = jnp.float32
BF16 = jnp.bfloat16
I32 = jnp.int32
SPLIT = 32
LAT, LON = "lat", "lon"
CHUNK = 256
LANES = 128
GRANT = 16 << 20
FULL = 59 << 20
META = 16

VMEM = pl.BlockSpec(memory_space=pltpu.VMEM)
SMEM = pl.BlockSpec(memory_space=pltpu.SMEM)
HBM = pl.BlockSpec(memory_space=pltpu.HBM)


def dot(a, b, ca=1, cb=0):
    return lax.dot_general(a, b, (((ca,), (cb,)), ((), ())), preferred_element_type=F32)


def turns(count):
    flips = sorted(range(count), key=lambda f: (-(f % 2 + f // 2), -f))
    shares = [f for k, f in enumerate(flips) if k % 4 in (0, 3)], [f for k, f in enumerate(flips) if k % 4 in (1, 2)]
    return list(zip(*sorted(shares, key=lambda share: share[-1])))


def cost(flops, nbytes):
    return pl.CostEstimate(flops=int(flops), bytes_accessed=int(nbytes), transcendentals=0)


def call(kernel, out_shape, specs, flops, scratch=(), grant=GRANT):
    many = isinstance(out_shape, list)
    return pl.pallas_call(
        kernel,
        out_shape=out_shape,
        in_specs=specs,
        out_specs=[VMEM] * len(out_shape) if many else VMEM,
        scratch_shapes=list(scratch),
        cost_estimate=cost(flops, 4 << 20),
        compiler_params=pltpu.CompilerParams(vmem_limit_bytes=grant),
    )


def silu(t):
    return 0.5 * t * (1.0 + jnp.tanh(0.5 * t))


def normed(raw, gain, offset, axis):
    width = raw.shape[axis]
    average = jnp.sum(raw, axis=axis, keepdims=True) * (1.0 / width)
    centred = raw - average
    spread = jnp.sum(centred * centred, axis=axis, keepdims=True) * (1.0 / width)
    return centred * lax.rsqrt(spread + 1e-05) * gain + offset


def columns_of(rows):
    height, width = rows.shape
    rows = rows.astype(F32)
    if height % 8:
        rows = jnp.concatenate([rows, jnp.zeros((8 - height % 8, width), F32)], 0)
    if width % LANES:
        rows = jnp.concatenate([rows, jnp.zeros((rows.shape[0], LANES - width % LANES), F32)], 1)
    return jnp.transpose(rows)


def open_kernel(
    lat_count,
    mesh_rows,
    owner_hbm,
    sender_hbm,
    node_hbm,
    feat_hbm,
    halo_hbm,
    from_hbm,
    to_hbm,
    latent,
    table_ref,
    meta_ref,
    ends_ref,
    asked_ref,
    base0,
    base1,
    base2,
    base3,
    owner_ref,
    sender_ref,
    node_ref,
    feat_ref,
    halo_ref,
    from_ref,
    to_ref,
    first_sem,
    sem,
):
    lon = lax.axis_index(LON)
    rows = base0.shape[0]
    inputs = (owner_hbm, sender_hbm, node_hbm, feat_hbm, halo_hbm, from_hbm, to_hbm)
    held = (owner_ref, sender_ref, node_ref, feat_ref, halo_ref, from_ref, to_ref)
    early = [pltpu.make_async_copy(a, b, first_sem.at[k]) for k, (a, b) in enumerate(zip(inputs, held))]
    late = []

    def bring(source, target):
        late.append(pltpu.make_async_copy(source, target, sem.at[len(late)]))

    for j, base in enumerate((base0, base1, base2, base3)):
        bring(latent.at[pl.ds(pl.multiple_of((lon ^ j) * rows, rows), rows), :], base)
    for copy in early + late:
        copy.start()
    for copy in early:
        copy.wait()
    ends_ref[...] = columns_of(jnp.concatenate([from_ref[...].astype(F32), to_ref[...].astype(F32)], 0)).astype(I32)
    asked = columns_of(halo_ref[...]).astype(I32)
    cap = halo_ref.shape[1]
    for p in range(lat_count):
        asked_ref[p * cap : (p + 1) * cap, :] = asked[0:cap, p : p + 1]
    edges = owner_ref.shape[1]
    owner = owner_ref[...]
    parts = lax.broadcasted_iota(I32, (lat_count, edges), 0)
    hits = jnp.where(parts == owner, 1.0, 0.0)
    lane = lax.broadcasted_iota(I32, (lat_count, edges), 1)
    count = hits
    step = 1
    while step < edges:
        count = count + jnp.where(lane >= step, pltpu.roll(count, step, 1), 0.0)
        step *= 2
    first = jnp.sum(jnp.where(owner < parts, 1.0, 0.0), axis=1, keepdims=True)
    place = jnp.sum(hits * (first + count - hits), axis=0, keepdims=True).astype(I32)
    key_rows = edges // LANES
    table_ref[key_rows:, :] = jnp.broadcast_to(first, (lat_count, LANES)).astype(I32)
    sender = sender_ref[...]
    node = node_ref[...]
    digits = [sender // SPLIT, sender % SPLIT, node // SPLIT, node % SPLIT, owner]
    rows = [d.astype(F32) for d in digits] + [feat_ref[...].astype(F32)]
    used = len(digits) + feat_ref.shape[0]
    meta = jnp.concatenate(rows + [jnp.ones((META - used, edges), F32)], 0).astype(BF16)
    for i in range(edges // CHUNK):
        spot = lax.broadcasted_iota(I32, (CHUNK, edges), 0) + i * CHUNK
        perm = jnp.where(spot == place, 1.0, 0.0).astype(BF16)
        moved = dot(meta, perm, 1, 1)
        meta_ref[:, i * CHUNK : (i + 1) * CHUNK] = moved.astype(BF16)
        key = moved[4:5] * float(mesh_rows) + moved[2:3] * float(SPLIT) + moved[3:4]
        for k in range(CHUNK // LANES):
            row = i * (CHUNK // LANES) + k
            table_ref[row : row + 1, :] = key[:, k * LANES : (k + 1) * LANES].astype(I32)
    for copy in late:
        copy.wait()


def message_kernel(n_feat, rows_ref, meta_ref, proj_ref, bias_ref, gain_ref, w0, w1, w2, w3, v0, v1, v2, v3, out_ref, win, wout, proj):
    quarter = w0.shape[1]
    lon = lax.axis_index(LON)
    for j, (w, v) in enumerate(((w0, v0), (w1, v1), (w2, v2), (w3, v3))):
        win[:, j * quarter : (j + 1) * quarter] = w[...]
        wout[:, j * quarter : (j + 1) * quarter] = v[...]
        at = pl.ds(pl.multiple_of((lon ^ j) * quarter, quarter), quarter)
        bias = bias_ref[0:1, at]
        high = bias.astype(BF16).astype(F32)
        mid = (bias - high).astype(BF16).astype(F32)
        low = bias - high - mid
        used = META - 5 - n_feat
        proj[:, j * quarter : (j + 1) * quarter] = jnp.concatenate(
            [jnp.zeros((5, quarter), F32), proj_ref[:, at].astype(F32), high, mid, low, jnp.zeros((used - 3, quarter), F32)], 0
        ).astype(BF16)
    rows = rows_ref[...]
    table = dot(rows, win[...]).astype(BF16)
    edges = meta_ref.shape[1]
    block = CHUNK
    for i in range(edges // block):
        at = slice(i * block, (i + 1) * block)
        places = jnp.transpose(meta_ref[:, at].astype(F32))
        meta = places.astype(BF16)
        sender = (places[:, 0:1] * float(SPLIT) + places[:, 1:2]).astype(I32)
        source = lax.broadcasted_iota(I32, (block, rows.shape[0]), 1)
        pick = jnp.where(source == sender, 1.0, 0.0).astype(BF16)
        pre = dot(pick, table) + dot(meta, proj[...])
        raw = dot(silu(pre).astype(BF16), wout[...], 1, 1)
        out_ref[at, :] = normed(raw, gain_ref[...], bias_ref[1:2, :], 1).astype(BF16)


def sums_kernel(mesh_rows, cap, keep, start_a, start_b, table_a, table_b, msg_a, msg_b, x_ref, y_ref):
    edges, _ = msg_a.shape
    key_rows = edges // LANES
    tall = y_ref.shape[1]
    quarter = mesh_rows // 4
    half = quarter // 2
    lat = lax.axis_index(LAT)
    low, high = lax.rem(lat, 2), lat // 2
    lon = lax.axis_index(LON)
    mine = lon * quarter
    other = (lon ^ 2) * quarter
    ready = min(key_rows, (cap + 2 * LANES - 2) // LANES)
    sets = ((start_a, table_a, msg_a), (start_b, table_b, msg_b))

    def sums(part, bases):
        rows = half * len(bases)
        row = lax.broadcasted_iota(I32, (rows, LANES), 0)
        node = row + (bases[0] + part * mesh_rows)
        for k in range(1, len(bases)):
            node = jnp.where(row >= k * half, row + (bases[k] - k * half + part * mesh_rows), node)

        total = None
        for start, table, msg in sets:
            at = jnp.minimum(start[key_rows + part, 0] // LANES, key_rows - ready)
            pick = jnp.concatenate(
                [jnp.where(node == table[pl.ds(at + k, 1), :], 1.0, 0.0).astype(BF16) for k in range(ready)], 1
            )
            term = dot(pick, msg[pl.ds(pl.multiple_of(at * LANES, LANES), ready * LANES), :])
            total = term if total is None else total + term
        return total.astype(BF16)

    near_low = low if keep else 1 - low
    base = mine if keep else other

    @pl.loop(0, tall, unroll=4)
    def _(i):
        both = sums(2 * i + near_low, (base, mine + half, other + half))
        one = sums(2 * i + 1 - near_low, (base,))
        to = i ^ high
        x_ref[0 if keep else 1, to] = both[:half]
        x_ref[1 if keep else 0, to] = one
        y_ref[0, to] = both[half : 2 * half]
        y_ref[1, to] = both[2 * half :]


def node_sums(keep, tables, messages, lat_count, mesh_rows):
    tall = lat_count // 2
    edges, width = messages[0].shape
    out = jax.ShapeDtypeStruct((2, tall, mesh_rows // 8, width), BF16)
    return call(
        functools.partial(sums_kernel, mesh_rows, 2 * edges // lat_count, keep), [out, out], [SMEM] * 2 + [VMEM] * 4, 2 * edges * mesh_rows * width
    )(*tables, *tables, *messages)


def join_kernel(keep_x, got_x, got_xy, keep_y, got_y, got_yx, *outs):
    half = keep_x.shape[2]
    for j, out in enumerate(outs):
        out[:half] = (keep_x[0, j].astype(F32) + got_x[0, j].astype(F32) + got_xy[j].astype(F32)).astype(BF16)
        out[half:] = (keep_y[0, j].astype(F32) + got_y[0, j].astype(F32) + got_yx[j].astype(F32)).astype(BF16)


def node_kernel(n_base, n_agg, n_out, *refs):
    bases, refs = refs[:n_base], refs[n_base:]
    aggs, refs = refs[:n_agg], refs[n_agg:]
    bias_ref, gain_ref = refs[:2]
    weights = refs[2:10]
    outs = refs[10 : 10 + n_out]
    base, win, wout = refs[10 + n_out :]
    width = base.shape[1]
    quarter = weights[0].shape[1]
    lon = lax.axis_index(LON)
    biases = []
    for j in range(4):
        win[:, j * quarter : (j + 1) * quarter] = weights[j][...]
        wout[j * quarter : (j + 1) * quarter, :] = weights[4 + j][...]
        at = pl.ds(pl.multiple_of((lon ^ j) * quarter, quarter), quarter)
        biases.append(bias_ref[0:1, at])
        if n_base > 1:
            base[:, at] = bases[j][...]
    if n_base == 1:
        base[...] = bases[0][...]
    total = None
    for ref in aggs:
        term = ref[...] if len(ref.shape) == 2 else ref[0]
        total = term.astype(F32) if total is None else total + term.astype(F32)
    own = base[...]
    pre = dot(own, win[0:width, :]) + dot(total.astype(BF16), win[width:, :]) + jnp.concatenate(biases, 1)
    raw = dot(silu(pre).astype(BF16), wout[...])
    new = (own.astype(F32) + normed(raw, gain_ref[...], bias_ref[1:2, :], 1)).astype(BF16)
    if n_out == 1:
        outs[0][...] = new
    else:
        base[...] = new
        for j in range(n_out):
            outs[j][...] = base[:, pl.ds(pl.multiple_of((lon ^ j) * quarter, quarter), quarter)]


def node_network(bases, aggregates, biases, gain, pieces, n_out):
    rows, width = bases[0].shape[0], gain.shape[0]
    quarter = pieces[0].shape[1]
    kernel = functools.partial(node_kernel, len(bases), len(aggregates), n_out)
    scratch = [pltpu.VMEM((rows, width), BF16), pltpu.VMEM((2 * width, width), BF16), pltpu.VMEM((width, width), BF16)]
    out = jax.ShapeDtypeStruct((rows, width if n_out == 1 else quarter), BF16)
    operands = (*bases, *aggregates, biases, gain[None, :], *pieces)
    return call(
        kernel, out if n_out == 1 else [out] * n_out, [VMEM] * len(operands), 6 * rows * width * width, scratch
    )(*operands)


def lay_kernel(*refs):
    pieces, out_ref = refs[:4], refs[4]
    rows = pieces[0].shape[0]
    for j in range(4):
        out_ref[pl.ds(pl.multiple_of((lax.axis_index(LON) ^ j) * rows, rows), rows), :] = pieces[j][...]


def pick_kernel(index_ref, table_ref, *refs):
    outs, held = refs[:-1], refs[-1]
    lane = lax.broadcasted_iota(I32, (index_ref.shape[0], table_ref.shape[0]), 1)
    pick = jnp.where(lane == index_ref[...], 1.0, 0.0).astype(BF16)
    held[...] = dot(pick, table_ref[...])
    cap = outs[0].shape[0]
    core = lax.rem(lax.axis_index(LON), 2)
    for out, (flip0, flip1) in zip(outs, turns(2 * len(outs))):
        at = (lax.axis_index(LAT) ^ jnp.where(core == 0, flip0, flip1)) * cap
        out[...] = held[pl.ds(pl.multiple_of(at, cap), cap), :].astype(BF16)


def pack_kernel(own_ref, *refs):
    out_ref = refs[-1]
    core = lax.rem(lax.axis_index(LON), 2)
    last = jnp.where(core == 0, own_ref[...].astype(F32), refs[-2][...].astype(F32))
    out_ref[...] = jnp.concatenate([ref[...].astype(F32) for ref in refs[:-2]] + [last], 0).astype(BF16)


def near_kernel(edge_hbm, mid_ref, ends_ref, bias_ref, w0, w1, w2, w3, out_ref, win, edge_ref, sem):
    block = CHUNK
    edges, width = edge_ref.shape
    loads = []
    for i in range(edges // block):
        at = pl.ds(i * block, block)
        loads.append(pltpu.make_async_copy(edge_hbm.at[at, :], edge_ref.at[at, :], sem.at[i]))
        loads[-1].start()
    quarter = w0.shape[1]
    lon = lax.axis_index(LON)
    biases = []
    for j, w in enumerate((w0, w1, w2, w3)):
        win[:, j * quarter : (j + 1) * quarter] = w[...]
        at = pl.ds(pl.multiple_of((lon ^ j) * quarter, quarter), quarter)
        biases.append(bias_ref[0:1, at])
    bias = jnp.concatenate(biases, 1)
    rows = mid_ref.shape[0]
    sent = dot(mid_ref[...], win[width : 2 * width, :]).astype(BF16)
    got = dot(mid_ref[...], win[2 * width :, :]).astype(BF16)
    for i in range(edges // block):
        at = slice(i * block, (i + 1) * block)
        lane = lax.broadcasted_iota(I32, (block, rows), 1)
        pick_s = jnp.where(lane == ends_ref[at, 0:1], 1.0, 0.0).astype(BF16)
        pick_r = jnp.where(lane == ends_ref[at, 1:2], 1.0, 0.0).astype(BF16)
        pre = dot(pick_s, sent) + dot(pick_r, got) + bias
        loads[i].wait()
        out_ref[at, :] = pre + dot(edge_ref[at, :], win[0:width, :])


def far_kernel(halo_cap, edge_hbm, pre_ref, halo_a, halo_b, ends_ref, receiver_ref, bias_ref, gain_ref, w0, w1, w2, w3, v0, v1, v2, v3, new_ref, away_ref, keep_ref, pass_ref, total, win, wout, edge_ref, sem):
    load = pltpu.make_async_copy(edge_hbm, edge_ref, sem)
    load.start()
    width = halo_a.shape[1]
    quarter = w0.shape[1]
    lon = lax.axis_index(LON)
    for j, (w, v) in enumerate(((w0, v0), (w1, v1), (w2, v2), (w3, v3))):
        win[:, j * quarter : (j + 1) * quarter] = w[width : 2 * width, :]
        wout[:, j * quarter : (j + 1) * quarter] = v[...]
    rows = halo_a.shape[0]
    mesh_rows = total.shape[0]
    sent = [dot(h[...], win[...]).astype(BF16) for h in (halo_a, halo_b)]
    lane = lax.broadcasted_iota(I32, (1, rows), 1)
    core = lax.rem(lon, 2)
    lat = lax.axis_index(LAT)
    flips = [jnp.zeros_like(lane), jnp.zeros_like(lane)]
    for j, pair in enumerate(turns(2 * (rows // halo_cap))):
        flips = [jnp.where(lane // halo_cap == j, flip, before) for flip, before in zip(pair, flips)]
    flips = [jnp.where(core == 0, a, b) for a, b in (flips, flips[::-1])]
    names = [mesh_rows + (lat ^ flip) * halo_cap + lane % halo_cap for flip in flips]
    edges = edge_ref.shape[0]
    block = 256
    for i in range(edges // block):
        at = slice(i * block, (i + 1) * block)
        pre = pre_ref[at, :]
        for name, rows_in in zip(names, sent):
            pick = jnp.where(name == ends_ref[at, 0:1], 1.0, 0.0).astype(BF16)
            pre = pre + dot(pick, rows_in)
        if i == 0:
            load.wait()
        raw = dot(silu(pre).astype(BF16), wout[...], 1, 1)
        new_ref[at, :] = (edge_ref[at, :].astype(F32) + normed(raw, gain_ref[...], bias_ref[1:2, :], 1)).astype(BF16)
    node = lax.broadcasted_iota(I32, (mesh_rows, edges), 0)
    onto = jnp.where(node == receiver_ref[...], 1.0, 0.0).astype(BF16)
    total[...] = dot(onto, new_ref[...]).astype(BF16)
    rows = keep_ref.shape[0]

    def part(flip):
        return total[pl.ds(pl.multiple_of((lon ^ flip) * rows, rows), rows), :]

    away_ref[0] = part(1)
    away_ref[1] = part(3)
    keep_ref[...] = part(0)
    pass_ref[...] = part(2)


def plus(*values):
    total = values[0].astype(F32)
    for v in values[1:]:
        total = total + v.astype(F32)
    return total.astype(BF16)


def local(
    grid_latent,
    grid_feat,
    grid_sender,
    grid_owner,
    grid_node,
    mesh_latent,
    mesh_edge,
    halo_send,
    mesh_sender,
    mesh_receiver,
    enc_edge_in,
    enc_feat_proj,
    enc_edge_out,
    enc_edge_bias,
    enc_edge_gain,
    enc_node_in,
    enc_node_out,
    enc_node_bias,
    enc_node_gain,
    proc_edge_in,
    proc_edge_out,
    proc_edge_bias,
    proc_edge_gain,
    proc_node_in,
    proc_node_out,
    proc_node_bias,
    proc_node_gain,
):
    lat_count = lax.axis_size(LAT)
    width = grid_latent.shape[1]
    quarter = mesh_latent.shape[1]
    mesh_rows = mesh_latent.shape[0]
    node_rows = mesh_rows // 4
    edges = grid_sender.shape[0]
    local_edges = mesh_edge.shape[0]
    halo_cap = halo_send.shape[1]
    listed = halo_send.size

    def like(rows, columns, kind=BF16):
        return jax.ShapeDtypeStruct((rows, columns), kind)

    def hop(values, axis, flip):
        size = lax.axis_size(axis)
        return lax.ppermute(values, axis, [(i, i ^ flip) for i in range(size)])

    def spread(shard):
        across = hop(shard, LON, 2)
        return (shard, hop(shard, LON, 1), across, hop(across, LON, 1))

    enc_in = spread(enc_edge_in)
    enc_out = spread(enc_edge_out)
    small = (grid_owner.reshape(1, edges), grid_sender[None, :], grid_node[None, :], grid_feat)
    small = small + (halo_send, mesh_sender[None, :], mesh_receiver[None, :])
    table, meta, ends, asked, *rest = call(
        functools.partial(open_kernel, lat_count, mesh_rows),
        [
            like(edges // LANES + lat_count, LANES, I32),
            like(META, edges),
            like(local_edges, 8, I32),
            like(listed, 1, I32),
        ]
        + [like(node_rows, quarter)] * 4,
        [HBM] * 8,
        2 * META * edges * edges * 8,
        [pltpu.VMEM(v.shape, v.dtype) for v in small]
        + [pltpu.SemaphoreType.DMA((len(small),)), pltpu.SemaphoreType.DMA((4,))],
        FULL,
    )(*small, mesh_latent)
    bases = tuple(rest[j] if j == 0 else hop(rest[j], LON, j) for j in range(4))
    node_pieces = spread(enc_node_in) + spread(enc_node_out)
    edge_in = spread(proc_edge_in)
    edge_out = spread(proc_edge_out)
    last_pieces = spread(proc_node_in) + spread(proc_node_out)

    tables = (table, hop(table, LON, 1))
    message = call(
        functools.partial(message_kernel, grid_feat.shape[0]),
        like(edges, width),
        [VMEM] * 13,
        4 * edges * width * width,
        [pltpu.VMEM((width, width), BF16), pltpu.VMEM((width, width), BF16), pltpu.VMEM((META, width), BF16)],
    )(grid_latent, meta, enc_feat_proj, enc_edge_bias, enc_edge_gain[None, :], *enc_in, *enc_out)
    messages = (message, hop(message, LON, 1))

    tall = lat_count // 2
    send_x, send_y = node_sums(False, tables, messages, lat_count, mesh_rows)
    got_x = hop(send_x, LON, 2)
    got_y = hop(send_y, LAT, 1)
    keep_x, keep_y = node_sums(True, tables, messages, lat_count, mesh_rows)
    got_xy = hop(plus(keep_x[1], got_x[1]), LAT, 1)
    got_yx = hop(plus(keep_y[1], got_y[1]), LON, 2)
    joined = call(join_kernel, [like(node_rows, width)] * tall, [VMEM] * 6, 1 << 20)(
        keep_x, got_x, got_xy, keep_y, got_y, got_yx
    )
    far_first = sorted(range(1, tall), key=lambda j: (j < tall // 2, j))
    partials = (joined[0], *[hop(joined[j], LAT, 2 * j) for j in far_first])

    mid = node_network(bases, partials, enc_node_bias, enc_node_gain, node_pieces, 1)
    mid_all = lax.all_gather(mid, LON, axis=0, tiled=True)

    picked = call(
        pick_kernel,
        [like(halo_cap, width)] * tall,
        [VMEM] * 2,
        2 * listed * mesh_rows * width,
        [pltpu.VMEM((listed, width), F32)],
    )(asked, mid_all)

    def halo_hop(j, flips):
        pairs = []
        for i in range(lat_count):
            for l in range(4):
                to = i ^ flips[l % 2]
                if to != i:
                    pairs.append((i * 4 + l, to * 4 + l))
        return lax.ppermute(picked[j], (LAT, LON), pairs)

    arrived = [halo_hop(j, flips) for j, flips in enumerate(turns(lat_count))]
    near = call(
        near_kernel,
        like(local_edges, width, F32),
        [HBM] + [VMEM] * 7,
        2 * local_edges * width * (width + 2 * mesh_rows),
        [
            pltpu.VMEM((3 * width, width), BF16),
            pltpu.VMEM((local_edges, width), BF16),
            pltpu.SemaphoreType.DMA((local_edges // CHUNK,)),
        ],
    )(mesh_edge, mid_all, ends, proc_edge_bias, *edge_in)
    packed = call(pack_kernel, like(listed // 2, width), [VMEM] * (tall + 1), 1 << 20)(picked[-1], *arrived)
    halves = (packed, hop(packed, LON, 1))

    edge_update, away, kept, passed = call(
        functools.partial(far_kernel, halo_cap),
        [
            like(local_edges, width),
            jax.ShapeDtypeStruct((2, node_rows, width), BF16),
            like(node_rows, width),
            like(node_rows, width),
        ],
        [HBM] + [VMEM] * 15,
        2 * local_edges * width * (width + listed + mesh_rows),
        [
            pltpu.VMEM((mesh_rows, width), BF16),
            pltpu.VMEM((width, width), BF16),
            pltpu.VMEM((width, width), BF16),
            pltpu.VMEM((local_edges, width), BF16),
            pltpu.SemaphoreType.DMA,
        ],
    )(mesh_edge, near, *halves, ends, mesh_receiver[None, :], proc_edge_bias, proc_edge_gain[None, :], *edge_in, *edge_out)

    came = hop(away, LON, 1)
    got = hop(plus(passed, came[1]), LON, 2)
    new = node_network((mid,), (kept, came, got), proc_node_bias, proc_node_gain, last_pieces, 4)
    mesh_update = call(lay_kernel, like(mesh_rows, quarter), [VMEM] * 4, 1 << 20)(
        new[0], *[hop(new[j], LON, j) for j in (1, 2, 3)]
    )
    return (mesh_update, edge_update)


def solution(mesh):
    both = (LAT, LON)
    placed = (
        P(both, None),
        P(None, both),
        P(both),
        P(both, None),
        P(both),
        P(LAT, LON),
        P(both, None),
        P(LAT, None),
        P(both),
        P(both),
        P(None, LON),
        P(),
        P(None, LON),
        P(),
        P(),
        P(None, LON),
        P(LON, None),
        P(),
        P(),
        P(None, LON),
        P(None, LON),
        P(),
        P(),
        P(None, LON),
        P(LON, None),
        P(),
        P(),
    )

    return jax.shard_map(
        local,
        mesh=mesh,
        in_specs=placed,
        out_specs=(P(LAT, LON), P(both, None)),
        check_vma=False,
    )
```

```python
import functools
import jax
import jax.numpy as jnp
from jax import lax
from jax.experimental import pallas as pl
from jax.experimental.pallas import tpu as pltpu
from jax.sharding import PartitionSpec as P


F32 = jnp.float32
BF16 = jnp.bfloat16
I32 = jnp.int32
SPLIT = 32
LAT, LON = "lat", "lon"
CHUNK = 256
LANES = 128
GRANT = 16 << 20
FULL = 59 << 20
META = 16

VMEM = pl.BlockSpec(memory_space=pltpu.VMEM)
SMEM = pl.BlockSpec(memory_space=pltpu.SMEM)
HBM = pl.BlockSpec(memory_space=pltpu.HBM)


def dot(a, b, ca=1, cb=0):
    return lax.dot_general(a, b, (((ca,), (cb,)), ((), ())), preferred_element_type=F32)


def turns(count):
    flips = sorted(range(count), key=lambda f: (-(f % 2 + f // 2), -f))
    shares = [f for k, f in enumerate(flips) if k % 4 in (0, 3)], [f for k, f in enumerate(flips) if k % 4 in (1, 2)]
    return list(zip(*sorted(shares, key=lambda share: share[-1])))


def cost(flops, nbytes):
    return pl.CostEstimate(flops=int(flops), bytes_accessed=int(nbytes), transcendentals=0)


def call(kernel, out_shape, specs, flops, scratch=(), grant=GRANT):
    many = isinstance(out_shape, list)
    return pl.pallas_call(
        kernel,
        out_shape=out_shape,
        in_specs=specs,
        out_specs=[VMEM] * len(out_shape) if many else VMEM,
        scratch_shapes=list(scratch),
        cost_estimate=cost(flops, 4 << 20),
        compiler_params=pltpu.CompilerParams(vmem_limit_bytes=grant),
    )


def silu(t):
    return 0.5 * t * (1.0 + jnp.tanh(0.5 * t))


def normed(raw, gain, offset, axis):
    width = raw.shape[axis]
    average = jnp.sum(raw, axis=axis, keepdims=True) * (1.0 / width)
    centred = raw - average
    spread = jnp.sum(centred * centred, axis=axis, keepdims=True) * (1.0 / width)
    return centred * lax.rsqrt(spread + 1e-05) * gain + offset


def columns_of(rows):
    height, width = rows.shape
    rows = rows.astype(F32)
    if height % 8:
        rows = jnp.concatenate([rows, jnp.zeros((8 - height % 8, width), F32)], 0)
    if width % LANES:
        rows = jnp.concatenate([rows, jnp.zeros((rows.shape[0], LANES - width % LANES), F32)], 1)
    return jnp.transpose(rows)


def open_kernel(
    lat_count,
    mesh_rows,
    owner_hbm,
    sender_hbm,
    node_hbm,
    feat_hbm,
    halo_hbm,
    from_hbm,
    to_hbm,
    latent,
    table_ref,
    meta_ref,
    ends_ref,
    asked_ref,
    base0,
    base1,
    base2,
    base3,
    owner_ref,
    sender_ref,
    node_ref,
    feat_ref,
    halo_ref,
    from_ref,
    to_ref,
    first_sem,
    sem,
):
    lon = lax.axis_index(LON)
    rows = base0.shape[0]
    inputs = (owner_hbm, sender_hbm, node_hbm, feat_hbm, halo_hbm, from_hbm, to_hbm)
    held = (owner_ref, sender_ref, node_ref, feat_ref, halo_ref, from_ref, to_ref)
    early = [pltpu.make_async_copy(a, b, first_sem.at[k]) for k, (a, b) in enumerate(zip(inputs, held))]
    late = []

    def bring(source, target):
        late.append(pltpu.make_async_copy(source, target, sem.at[len(late)]))

    for j, base in enumerate((base0, base1, base2, base3)):
        bring(latent.at[pl.ds(pl.multiple_of((lon ^ j) * rows, rows), rows), :], base)
    for copy in early + late:
        copy.start()
    for copy in early:
        copy.wait()
    ends_ref[...] = columns_of(jnp.concatenate([from_ref[...].astype(F32), to_ref[...].astype(F32)], 0)).astype(I32)
    asked = columns_of(halo_ref[...]).astype(I32)
    cap = halo_ref.shape[1]
    for p in range(lat_count):
        asked_ref[p * cap : (p + 1) * cap, :] = asked[0:cap, p : p + 1]
    edges = owner_ref.shape[1]
    owner = owner_ref[...]
    parts = lax.broadcasted_iota(I32, (lat_count, edges), 0)
    hits = jnp.where(parts == owner, 1.0, 0.0)
    lane = lax.broadcasted_iota(I32, (lat_count, edges), 1)
    count = hits
    step = 1
    while step < edges:
        count = count + jnp.where(lane >= step, pltpu.roll(count, step, 1), 0.0)
        step *= 2
    first = jnp.sum(jnp.where(owner < parts, 1.0, 0.0), axis=1, keepdims=True)
    place = jnp.sum(hits * (first + count - hits), axis=0, keepdims=True).astype(I32)
    key_rows = edges // LANES
    table_ref[key_rows:, :] = jnp.broadcast_to(first, (lat_count, LANES)).astype(I32)
    sender = sender_ref[...]
    node = node_ref[...]
    digits = [sender // SPLIT, sender % SPLIT, node // SPLIT, node % SPLIT, owner]
    rows = [d.astype(F32) for d in digits] + [feat_ref[...].astype(F32)]
    used = len(digits) + feat_ref.shape[0]
    meta = jnp.concatenate(rows + [jnp.ones((META - used, edges), F32)], 0).astype(BF16)
    for i in range(edges // CHUNK):
        spot = lax.broadcasted_iota(I32, (CHUNK, edges), 0) + i * CHUNK
        perm = jnp.where(spot == place, 1.0, 0.0).astype(BF16)
        moved = dot(meta, perm, 1, 1)
        meta_ref[:, i * CHUNK : (i + 1) * CHUNK] = moved.astype(BF16)
        key = moved[4:5] * float(mesh_rows) + moved[2:3] * float(SPLIT) + moved[3:4]
        for k in range(CHUNK // LANES):
            row = i * (CHUNK // LANES) + k
            table_ref[row : row + 1, :] = key[:, k * LANES : (k + 1) * LANES].astype(I32)
    for copy in late:
        copy.wait()


def message_kernel(n_feat, rows_ref, meta_ref, proj_ref, bias_ref, gain_ref, w0, w1, w2, w3, v0, v1, v2, v3, out_ref, win, wout, proj):
    quarter = w0.shape[1]
    lon = lax.axis_index(LON)
    for j, (w, v) in enumerate(((w0, v0), (w1, v1), (w2, v2), (w3, v3))):
        win[:, j * quarter : (j + 1) * quarter] = w[...]
        wout[:, j * quarter : (j + 1) * quarter] = v[...]
        at = pl.ds(pl.multiple_of((lon ^ j) * quarter, quarter), quarter)
        bias = bias_ref[0:1, at]
        high = bias.astype(BF16).astype(F32)
        mid = (bias - high).astype(BF16).astype(F32)
        low = bias - high - mid
        used = META - 5 - n_feat
        proj[:, j * quarter : (j + 1) * quarter] = jnp.concatenate(
            [jnp.zeros((5, quarter), F32), proj_ref[:, at].astype(F32), high, mid, low, jnp.zeros((used - 3, quarter), F32)], 0
        ).astype(BF16)
    rows = rows_ref[...]
    table = dot(rows, win[...]).astype(BF16)
    edges = meta_ref.shape[1]
    block = 4 * CHUNK
    for i in range(edges // block):
        at = slice(i * block, (i + 1) * block)
        places = jnp.transpose(meta_ref[:, at].astype(F32))
        meta = places.astype(BF16)
        sender = (places[:, 0:1] * float(SPLIT) + places[:, 1:2]).astype(I32)
        source = lax.broadcasted_iota(I32, (block, rows.shape[0]), 1)
        pick = jnp.where(source == sender, 1.0, 0.0).astype(BF16)
        pre = dot(pick, table) + dot(meta, proj[...])
        raw = dot(silu(pre).astype(BF16), wout[...], 1, 1)
        out_ref[at, :] = normed(raw, gain_ref[...], bias_ref[1:2, :], 1).astype(BF16)


def sums_kernel(mesh_rows, cap, keep, start_a, start_b, table_a, table_b, msg_a, msg_b, x_ref, y_ref):
    edges, _ = msg_a.shape
    key_rows = edges // LANES
    tall = y_ref.shape[1]
    quarter = mesh_rows // 4
    half = quarter // 2
    lat = lax.axis_index(LAT)
    low, high = lax.rem(lat, 2), lat // 2
    lon = lax.axis_index(LON)
    mine = lon * quarter
    other = (lon ^ 2) * quarter
    ready = min(key_rows, (cap + 2 * LANES - 2) // LANES)
    sets = ((start_a, table_a, msg_a), (start_b, table_b, msg_b))

    def sums(part, bases):
        rows = half * len(bases)
        row = lax.broadcasted_iota(I32, (rows, LANES), 0)
        node = row + (bases[0] + part * mesh_rows)
        for k in range(1, len(bases)):
            node = jnp.where(row >= k * half, row + (bases[k] - k * half + part * mesh_rows), node)

        total = None
        for start, table, msg in sets:
            at = jnp.minimum(start[key_rows + part, 0] // LANES, key_rows - ready)
            pick = jnp.concatenate(
                [jnp.where(node == table[pl.ds(at + k, 1), :], 1.0, 0.0).astype(BF16) for k in range(ready)], 1
            )
            term = dot(pick, msg[pl.ds(pl.multiple_of(at * LANES, LANES), ready * LANES), :])
            total = term if total is None else total + term
        return total.astype(BF16)

    near_low = low if keep else 1 - low
    base = mine if keep else other

    @pl.loop(0, tall, unroll=4)
    def _(i):
        both = sums(2 * i + near_low, (base, mine + half, other + half))
        one = sums(2 * i + 1 - near_low, (base,))
        to = i ^ high
        x_ref[0 if keep else 1, to] = both[:half]
        x_ref[1 if keep else 0, to] = one
        y_ref[0, to] = both[half : 2 * half]
        y_ref[1, to] = both[2 * half :]


def node_sums(keep, tables, messages, lat_count, mesh_rows):
    tall = lat_count // 2
    edges, width = messages[0].shape
    out = jax.ShapeDtypeStruct((2, tall, mesh_rows // 8, width), BF16)
    return call(
        functools.partial(sums_kernel, mesh_rows, 2 * edges // lat_count, keep), [out, out], [SMEM] * 2 + [VMEM] * 4, 2 * edges * mesh_rows * width
    )(*tables, *tables, *messages)


def join_kernel(keep_x, got_x, got_xy, keep_y, got_y, got_yx, *outs):
    half = keep_x.shape[2]
    for j, out in enumerate(outs):
        out[:half] = (keep_x[0, j].astype(F32) + got_x[0, j].astype(F32) + got_xy[j].astype(F32)).astype(BF16)
        out[half:] = (keep_y[0, j].astype(F32) + got_y[0, j].astype(F32) + got_yx[j].astype(F32)).astype(BF16)


def node_kernel(n_base, n_agg, n_out, *refs):
    bases, refs = refs[:n_base], refs[n_base:]
    aggs, refs = refs[:n_agg], refs[n_agg:]
    bias_ref, gain_ref = refs[:2]
    weights = refs[2:10]
    outs = refs[10 : 10 + n_out]
    base, win, wout = refs[10 + n_out :]
    width = base.shape[1]
    quarter = weights[0].shape[1]
    lon = lax.axis_index(LON)
    biases = []
    for j in range(4):
        win[:, j * quarter : (j + 1) * quarter] = weights[j][...]
        wout[j * quarter : (j + 1) * quarter, :] = weights[4 + j][...]
        at = pl.ds(pl.multiple_of((lon ^ j) * quarter, quarter), quarter)
        biases.append(bias_ref[0:1, at])
        if n_base > 1:
            base[:, at] = bases[j][...]
    if n_base == 1:
        base[...] = bases[0][...]
    total = None
    for ref in aggs:
        term = ref[...] if len(ref.shape) == 2 else ref[0]
        total = term.astype(F32) if total is None else total + term.astype(F32)
    own = base[...]
    pre = dot(own, win[0:width, :]) + dot(total.astype(BF16), win[width:, :]) + jnp.concatenate(biases, 1)
    raw = dot(silu(pre).astype(BF16), wout[...])
    new = (own.astype(F32) + normed(raw, gain_ref[...], bias_ref[1:2, :], 1)).astype(BF16)
    if n_out == 1:
        outs[0][...] = new
    else:
        base[...] = new
        for j in range(n_out):
            outs[j][...] = base[:, pl.ds(pl.multiple_of((lon ^ j) * quarter, quarter), quarter)]


def node_network(bases, aggregates, biases, gain, pieces, n_out):
    rows, width = bases[0].shape[0], gain.shape[0]
    quarter = pieces[0].shape[1]
    kernel = functools.partial(node_kernel, len(bases), len(aggregates), n_out)
    scratch = [pltpu.VMEM((rows, width), BF16), pltpu.VMEM((2 * width, width), BF16), pltpu.VMEM((width, width), BF16)]
    out = jax.ShapeDtypeStruct((rows, width if n_out == 1 else quarter), BF16)
    operands = (*bases, *aggregates, biases, gain[None, :], *pieces)
    return call(
        kernel, out if n_out == 1 else [out] * n_out, [VMEM] * len(operands), 6 * rows * width * width, scratch
    )(*operands)


def lay_kernel(*refs):
    pieces, out_ref = refs[:4], refs[4]
    rows = pieces[0].shape[0]
    for j in range(4):
        out_ref[pl.ds(pl.multiple_of((lax.axis_index(LON) ^ j) * rows, rows), rows), :] = pieces[j][...]


def pick_kernel(index_ref, table_ref, *refs):
    outs, held = refs[:-1], refs[-1]
    lane = lax.broadcasted_iota(I32, (index_ref.shape[0], table_ref.shape[0]), 1)
    pick = jnp.where(lane == index_ref[...], 1.0, 0.0).astype(BF16)
    held[...] = dot(pick, table_ref[...])
    cap = outs[0].shape[0]
    core = lax.rem(lax.axis_index(LON), 2)
    for out, (flip0, flip1) in zip(outs, turns(2 * len(outs))):
        at = (lax.axis_index(LAT) ^ jnp.where(core == 0, flip0, flip1)) * cap
        out[...] = held[pl.ds(pl.multiple_of(at, cap), cap), :].astype(BF16)


def pack_kernel(own_ref, *refs):
    out_ref = refs[-1]
    core = lax.rem(lax.axis_index(LON), 2)
    last = jnp.where(core == 0, own_ref[...].astype(F32), refs[-2][...].astype(F32))
    out_ref[...] = jnp.concatenate([ref[...].astype(F32) for ref in refs[:-2]] + [last], 0).astype(BF16)


def near_kernel(edge_hbm, mid_ref, ends_ref, bias_ref, w0, w1, w2, w3, out_ref, win, edge_ref, sem):
    block = 2 * CHUNK
    edges, width = edge_ref.shape
    loads = []
    for i in range(edges // block):
        at = pl.ds(i * block, block)
        loads.append(pltpu.make_async_copy(edge_hbm.at[at, :], edge_ref.at[at, :], sem.at[i]))
        loads[-1].start()
    quarter = w0.shape[1]
    lon = lax.axis_index(LON)
    biases = []
    for j, w in enumerate((w0, w1, w2, w3)):
        win[:, j * quarter : (j + 1) * quarter] = w[...]
        at = pl.ds(pl.multiple_of((lon ^ j) * quarter, quarter), quarter)
        biases.append(bias_ref[0:1, at])
    bias = jnp.concatenate(biases, 1)
    rows = mid_ref.shape[0]
    sent = dot(mid_ref[...], win[width : 2 * width, :]).astype(BF16)
    got = dot(mid_ref[...], win[2 * width :, :]).astype(BF16)
    for i in range(edges // block):
        at = slice(i * block, (i + 1) * block)
        lane = lax.broadcasted_iota(I32, (block, rows), 1)
        pick_s = jnp.where(lane == ends_ref[at, 0:1], 1.0, 0.0).astype(BF16)
        pick_r = jnp.where(lane == ends_ref[at, 1:2], 1.0, 0.0).astype(BF16)
        pre = dot(pick_s, sent) + dot(pick_r, got) + bias
        loads[i].wait()
        out_ref[at, :] = pre + dot(edge_ref[at, :], win[0:width, :])


def far_kernel(halo_cap, edge_hbm, pre_ref, halo_a, halo_b, ends_ref, receiver_ref, bias_ref, gain_ref, w0, w1, w2, w3, v0, v1, v2, v3, new_ref, away_ref, keep_ref, pass_ref, total, win, wout, edge_ref, sem):
    load = pltpu.make_async_copy(edge_hbm, edge_ref, sem)
    load.start()
    width = halo_a.shape[1]
    quarter = w0.shape[1]
    lon = lax.axis_index(LON)
    for j, (w, v) in enumerate(((w0, v0), (w1, v1), (w2, v2), (w3, v3))):
        win[:, j * quarter : (j + 1) * quarter] = w[width : 2 * width, :]
        wout[:, j * quarter : (j + 1) * quarter] = v[...]
    rows = halo_a.shape[0]
    mesh_rows = total.shape[0]
    sent = [dot(h[...], win[...]).astype(BF16) for h in (halo_a, halo_b)]
    lane = lax.broadcasted_iota(I32, (1, rows), 1)
    core = lax.rem(lon, 2)
    lat = lax.axis_index(LAT)
    flips = [jnp.zeros_like(lane), jnp.zeros_like(lane)]
    for j, pair in enumerate(turns(2 * (rows // halo_cap))):
        flips = [jnp.where(lane // halo_cap == j, flip, before) for flip, before in zip(pair, flips)]
    flips = [jnp.where(core == 0, a, b) for a, b in (flips, flips[::-1])]
    names = [mesh_rows + (lat ^ flip) * halo_cap + lane % halo_cap for flip in flips]
    edges = edge_ref.shape[0]
    block = 2 * CHUNK
    for i in range(edges // block):
        at = slice(i * block, (i + 1) * block)
        pre = pre_ref[at, :]
        for name, rows_in in zip(names, sent):
            pick = jnp.where(name == ends_ref[at, 0:1], 1.0, 0.0).astype(BF16)
            pre = pre + dot(pick, rows_in)
        if i == 0:
            load.wait()
        raw = dot(silu(pre).astype(BF16), wout[...], 1, 1)
        new_ref[at, :] = (edge_ref[at, :].astype(F32) + normed(raw, gain_ref[...], bias_ref[1:2, :], 1)).astype(BF16)
    node = lax.broadcasted_iota(I32, (mesh_rows, edges), 0)
    onto = jnp.where(node == receiver_ref[...], 1.0, 0.0).astype(BF16)
    total[...] = dot(onto, new_ref[...]).astype(BF16)
    rows = keep_ref.shape[0]

    def part(flip):
        return total[pl.ds(pl.multiple_of((lon ^ flip) * rows, rows), rows), :]

    away_ref[0] = part(1)
    away_ref[1] = part(3)
    keep_ref[...] = part(0)
    pass_ref[...] = part(2)


def plus(*values):
    total = values[0].astype(F32)
    for v in values[1:]:
        total = total + v.astype(F32)
    return total.astype(BF16)


def local(
    grid_latent,
    grid_feat,
    grid_sender,
    grid_owner,
    grid_node,
    mesh_latent,
    mesh_edge,
    halo_send,
    mesh_sender,
    mesh_receiver,
    enc_edge_in,
    enc_feat_proj,
    enc_edge_out,
    enc_edge_bias,
    enc_edge_gain,
    enc_node_in,
    enc_node_out,
    enc_node_bias,
    enc_node_gain,
    proc_edge_in,
    proc_edge_out,
    proc_edge_bias,
    proc_edge_gain,
    proc_node_in,
    proc_node_out,
    proc_node_bias,
    proc_node_gain,
):
    lat_count = lax.axis_size(LAT)
    width = grid_latent.shape[1]
    quarter = mesh_latent.shape[1]
    mesh_rows = mesh_latent.shape[0]
    node_rows = mesh_rows // 4
    edges = grid_sender.shape[0]
    local_edges = mesh_edge.shape[0]
    halo_cap = halo_send.shape[1]
    listed = halo_send.size

    def like(rows, columns, kind=BF16):
        return jax.ShapeDtypeStruct((rows, columns), kind)

    def hop(values, axis, flip):
        size = lax.axis_size(axis)
        return lax.ppermute(values, axis, [(i, i ^ flip) for i in range(size)])

    def spread(shard):
        across = hop(shard, LON, 2)
        return (shard, hop(shard, LON, 1), across, hop(across, LON, 1))

    enc_in = spread(enc_edge_in)
    enc_out = spread(enc_edge_out)
    small = (grid_owner.reshape(1, edges), grid_sender[None, :], grid_node[None, :], grid_feat)
    small = small + (halo_send, mesh_sender[None, :], mesh_receiver[None, :])
    table, meta, ends, asked, *rest = call(
        functools.partial(open_kernel, lat_count, mesh_rows),
        [
            like(edges // LANES + lat_count, LANES, I32),
            like(META, edges),
            like(local_edges, 8, I32),
            like(listed, 1, I32),
        ]
        + [like(node_rows, quarter)] * 4,
        [HBM] * 8,
        2 * META * edges * edges * 8,
        [pltpu.VMEM(v.shape, v.dtype) for v in small]
        + [pltpu.SemaphoreType.DMA((len(small),)), pltpu.SemaphoreType.DMA((4,))],
        FULL,
    )(*small, mesh_latent)
    bases = tuple(rest[j] if j == 0 else hop(rest[j], LON, j) for j in range(4))
    node_pieces = spread(enc_node_in) + spread(enc_node_out)
    edge_in = spread(proc_edge_in)
    edge_out = spread(proc_edge_out)
    last_pieces = spread(proc_node_in) + spread(proc_node_out)

    tables = (table, hop(table, LON, 1))
    message = call(
        functools.partial(message_kernel, grid_feat.shape[0]),
        like(edges, width),
        [VMEM] * 13,
        4 * edges * width * width,
        [pltpu.VMEM((width, width), BF16), pltpu.VMEM((width, width), BF16), pltpu.VMEM((META, width), BF16)],
    )(grid_latent, meta, enc_feat_proj, enc_edge_bias, enc_edge_gain[None, :], *enc_in, *enc_out)
    messages = (message, hop(message, LON, 1))

    tall = lat_count // 2
    send_x, send_y = node_sums(False, tables, messages, lat_count, mesh_rows)
    got_x = hop(send_x, LON, 2)
    got_y = hop(send_y, LAT, 1)
    keep_x, keep_y = node_sums(True, tables, messages, lat_count, mesh_rows)
    got_xy = hop(plus(keep_x[1], got_x[1]), LAT, 1)
    got_yx = hop(plus(keep_y[1], got_y[1]), LON, 2)
    joined = call(join_kernel, [like(node_rows, width)] * tall, [VMEM] * 6, 1 << 20)(
        keep_x, got_x, got_xy, keep_y, got_y, got_yx
    )
    far_first = sorted(range(1, tall), key=lambda j: (j < tall // 2, j))
    partials = (joined[0], *[hop(joined[j], LAT, 2 * j) for j in far_first])

    mid = node_network(bases, partials, enc_node_bias, enc_node_gain, node_pieces, 1)
    mid_all = lax.all_gather(mid, LON, axis=0, tiled=True)

    picked = call(
        pick_kernel,
        [like(halo_cap, width)] * tall,
        [VMEM] * 2,
        2 * listed * mesh_rows * width,
        [pltpu.VMEM((listed, width), F32)],
    )(asked, mid_all)

    def halo_hop(j, flips):
        pairs = []
        for i in range(lat_count):
            for l in range(4):
                to = i ^ flips[l % 2]
                if to != i:
                    pairs.append((i * 4 + l, to * 4 + l))
        return lax.ppermute(picked[j], (LAT, LON), pairs)

    arrived = [halo_hop(j, flips) for j, flips in enumerate(turns(lat_count))]
    near = call(
        near_kernel,
        like(local_edges, width, F32),
        [HBM] + [VMEM] * 7,
        2 * local_edges * width * (width + 2 * mesh_rows),
        [
            pltpu.VMEM((3 * width, width), BF16),
            pltpu.VMEM((local_edges, width), BF16),
            pltpu.SemaphoreType.DMA((local_edges // CHUNK,)),
        ],
    )(mesh_edge, mid_all, ends, proc_edge_bias, *edge_in)
    packed = call(pack_kernel, like(listed // 2, width), [VMEM] * (tall + 1), 1 << 20)(picked[-1], *arrived)
    halves = (packed, hop(packed, LON, 1))

    edge_update, away, kept, passed = call(
        functools.partial(far_kernel, halo_cap),
        [
            like(local_edges, width),
            jax.ShapeDtypeStruct((2, node_rows, width), BF16),
            like(node_rows, width),
            like(node_rows, width),
        ],
        [HBM] + [VMEM] * 15,
        2 * local_edges * width * (width + listed + mesh_rows),
        [
            pltpu.VMEM((mesh_rows, width), BF16),
            pltpu.VMEM((width, width), BF16),
            pltpu.VMEM((width, width), BF16),
            pltpu.VMEM((local_edges, width), BF16),
            pltpu.SemaphoreType.DMA,
        ],
    )(mesh_edge, near, *halves, ends, mesh_receiver[None, :], proc_edge_bias, proc_edge_gain[None, :], *edge_in, *edge_out)

    came = hop(away, LON, 1)
    got = hop(plus(passed, came[1]), LON, 2)
    new = node_network((mid,), (kept, came, got), proc_node_bias, proc_node_gain, last_pieces, 4)
    mesh_update = call(lay_kernel, like(mesh_rows, quarter), [VMEM] * 4, 1 << 20)(
        new[0], *[hop(new[j], LON, j) for j in (1, 2, 3)]
    )
    return (mesh_update, edge_update)


def solution(mesh):
    both = (LAT, LON)
    placed = (
        P(both, None),
        P(None, both),
        P(both),
        P(both, None),
        P(both),
        P(LAT, LON),
        P(both, None),
        P(LAT, None),
        P(both),
        P(both),
        P(None, LON),
        P(),
        P(None, LON),
        P(),
        P(),
        P(None, LON),
        P(LON, None),
        P(),
        P(),
        P(None, LON),
        P(None, LON),
        P(),
        P(),
        P(None, LON),
        P(LON, None),
        P(),
        P(),
    )

    return jax.shard_map(
        local,
        mesh=mesh,
        in_specs=placed,
        out_specs=(P(LAT, LON), P(both, None)),
        check_vma=False,
    )
```
